512 devices in a mesh: src: 64 (over z, y), ccd: 8 (over x, core).
Axes of the slice: x: 4, y: 4, z: 16, core: 2. Of those that a mesh axis runs over, the one named last changes fastest.
Arguments:
- design: float32 [5, 4194304], P(None, ('src', 'ccd')), may hold values from -6 to 6
- observed: float32 [4194304], P(('src', 'ccd')), may hold values from -12 to 12
- weight: float32 [4194304], P(('src', 'ccd')), may hold values from 0.25 to 4
- phase_frac: float32 [4194304], P(('src', 'ccd')), may hold values from 0 to 1
- axis_factors: float32 [3, 4194304], P(None, ('src', 'ccd')), may hold values from -6 to 6
- source_index: int32 [4194304], P(('src', 'ccd')), may hold values from 0 to 1023
- knot_index: int32 [4194304], P(('src', 'ccd')), may hold values from 0 to 127
- counts: int32 [64, 8, 64], P('src', 'ccd'), may hold values from 1 to 128, as said below
Outputs:
- source_params: float32 [5, 65536], P(None, 'src')
- attitude: float32 [3, 8192], P(None, 'src')
- residual: float32 [4194304], P(('src', 'ccd'))
The draws below stay inside these ranges and needn't reach their ends.
Inputs may be any that keep to these rules, and one draw needn't show every extreme that they name: Slot l of device (p, c) is live when l % 128 < counts[p, c, l // 128]; every device has one full block of 128 live slots, and one time shard receives full blocks from every device.
All inputs are finite; a program needn't handle non-finite values.
Results may differ from the reference program's by a relative error of at most 0.0003.
Values sent between devices are 32-bit elements; how exact they have to be, the bound alone decides.
A program may use at most 64 MiB of HBM per device.

```python
import math
import jax
import jax.numpy as jnp
from jax import lax

ROWS_DEV = 8192
SRC_DEV = 1024
KNOT_DEV = 128
ITERS = 3
SHARDS = 64
CCDS = 8
CAP = 128
KNOTS = 8192
ROWS = 4194304
N_SRC = 64
N_CCD = 8


def draw_counts(key, part):
    subkeys = jax.random.split(jax.random.fold_in(key, 7), 5)
    shape_all = (SHARDS, CCDS, SHARDS)
    heavy_dest = jax.random.randint(subkeys[0], (SHARDS,), 0, 4) == 0
    light_load = jax.random.randint(subkeys[1], shape_all, 1, CAP // 4 + 2)
    heavy_load = jax.random.randint(subkeys[2], shape_all, max(CAP // 2, 1), CAP + 1)
    block_loads = jnp.where(heavy_dest[None, None, :], heavy_load, light_load)
    full_dest = jax.random.randint(subkeys[3], (), 0, SHARDS)
    offset = jax.random.randint(subkeys[4], (), 1, SHARDS)
    sender = lax.broadcasted_iota(jnp.int32, shape_all, 0)
    target = lax.broadcasted_iota(jnp.int32, shape_all, 2)
    full_block = (target == full_dest) | (target == (sender + offset) % SHARDS)
    return jnp.minimum(jnp.where(full_block, CAP, block_loads), CAP).astype(jnp.int32)


def set_ends(drawn, rng, smallest, top_value):
    spot = [jax.random.randint(jax.random.fold_in(rng, axis), (), 0, length) for axis, length in enumerate(drawn.shape)]
    widest = drawn.shape.index(max(drawn.shape))
    beside = spot[:widest] + [(spot[widest] + 1) % drawn.shape[widest]] + spot[widest + 1:]
    return drawn.at[tuple(spot)].set(smallest).at[tuple(beside)].set(top_value)


def block_levels(key, shape, cuts, smallest, top_value):
    def one(dim, blocks):
        steps = jax.random.uniform(jax.random.fold_in(jax.random.fold_in(key, 6), dim), (blocks,), jnp.float32, smallest / len(cuts), top_value / len(cuts))
        return jnp.repeat(jnp.exp(steps), shape[dim] // blocks).reshape((-1,) + (1,) * (len(shape) - dim - 1))

    factor_of = one(*cuts[0])
    for cut in cuts[1:]:
        factor_of = factor_of * one(*cut)
    return factor_of


def noise(rng, shape, deviation, limit, pieces=(), kind=jnp.bfloat16):
    drawn = deviation * jax.random.normal(rng, shape, jnp.float32)
    if pieces:
        drawn = drawn * block_levels(rng, shape, pieces, -0.22, 0.18)
    return jnp.clip(drawn, -limit, limit).astype(kind)


def setup_inputs(seed: int = 0) -> dict:
    seeds = jax.random.split(jax.random.key(seed), 9)
    design = noise(seeds[0], (5, ROWS), 1.0, 6.0, ((1, 512),), jnp.float32)
    observed = noise(seeds[1], (ROWS,), 2.0, 12.0, ((0, 512),), jnp.float32)
    weight = jnp.clip(jnp.exp(math.log(4.0) - 2.7725887 * jax.random.uniform(seeds[2], (ROWS,), jnp.float32) ** block_levels(seeds[2], (ROWS,), ((0, 512),), -0.2, 0.2)), 0.25, 4.0)
    phase_frac = jnp.clip(1.0 * jax.random.uniform(seeds[3], (ROWS,), jnp.float32) ** block_levels(seeds[3], (ROWS,), ((0, 512),), -0.2, 0.2), 0.0, 1.0)
    axis_factors = noise(seeds[4], (3, ROWS), 1.0, 6.0, ((1, 512),), jnp.float32)
    source_index = set_ends(jax.random.randint(seeds[5], (ROWS,), 0, SRC_DEV), jax.random.fold_in(seeds[5], 1), 0, SRC_DEV - 1).astype(jnp.int32)
    knot_index = set_ends(jax.random.randint(seeds[6], (ROWS,), 0, KNOT_DEV), jax.random.fold_in(seeds[6], 1), 0, KNOT_DEV - 1).astype(jnp.int32)
    counts = draw_counts(jax.random.fold_in(seeds[8], 71), 0)
    return dict(design=design, observed=observed, weight=weight, phase_frac=phase_frac, axis_factors=axis_factors, source_index=source_index, knot_index=knot_index, counts=counts)


src_ridge = 1.0
att_ridge = 1.0
relax_step = 0.15

def row_moments(design_rows, observed_rows, weight_rows):
    products = []
    for m in range(5):
        for n in range(m, 5):
            products.append(design_rows[m] * design_rows[n] * weight_rows)
    for m in range(5):
        products.append(design_rows[m] * weight_rows * observed_rows)
    return jnp.stack(products)

def solve_small(moments):
    matrix = {}
    position = 0
    for m in range(5):
        for n in range(m, 5):
            matrix[m, n] = moments[position] + (src_ridge if m == n else 0.0)
            position += 1
    factor = {}
    for j in range(5):
        for i in range(j, 5):
            running = matrix[j, i]
            for k in range(j):
                running = running - factor[i, k] * factor[j, k]
            if i == j:
                factor[j, j] = jnp.sqrt(running)
            else:
                factor[i, j] = running / factor[j, j]
    forward = []
    for i in range(5):
        running = moments[15 + i]
        for k in range(i):
            running = running - factor[i, k] * forward[k]
        forward.append(running / factor[i, i])
    solution = [None] * 5
    for i in reversed(range(5)):
        running = forward[i]
        for k in range(i + 1, 5):
            running = running - factor[k, i] * solution[k]
        solution[i] = running / factor[i, i]
    return jnp.stack(solution)

def spline_basis(phase_rows):
    remain = 1.0 - phase_rows
    square = phase_rows * phase_rows
    cube_term = square * phase_rows
    return [remain * remain * remain / 6.0, (3.0 * cube_term - 6.0 * square + 4.0) / 6.0, (-3.0 * cube_term + 3.0 * square + 3.0 * phase_rows + 1.0) / 6.0, cube_term / 6.0]

def spread_ref(row_values, spline_terms, knot_rows):
    running = jnp.zeros((3, KNOTS + 3), jnp.float32)
    for j in range(4):
        running = running + jax.ops.segment_sum((row_values * spline_terms[j]).T, knot_rows + j, num_segments=KNOTS + 3).T
    return running

def predict_ref(padded, spline_terms, axis_rows, knot_rows):
    running = jnp.zeros_like(spline_terms[0])
    for j in range(4):
        running = running + spline_terms[j] * lax.optimization_barrier(jnp.sum(axis_rows * jnp.take(padded, knot_rows + j, axis=1), 0))
    return running

def reference(design, observed, weight, phase_frac, axis_factors, source_index, knot_index, counts):
    shard_rows = N_CCD * ROWS_DEV
    local_row = jnp.arange(ROWS_DEV, dtype=jnp.int32)
    bucket = local_row // CAP
    slot_pos = local_row % CAP
    live_mask = (slot_pos[None, None, :] < counts[:, :, bucket]).astype(jnp.float32).reshape(N_SRC, shard_rows)
    design_sh = design.reshape(5, N_SRC, shard_rows).transpose(1, 0, 2)
    factor_sh = axis_factors.reshape(3, N_SRC, shard_rows).transpose(1, 0, 2)
    observed_sh = observed.reshape(N_SRC, shard_rows)
    weight_sh = weight.reshape(N_SRC, shard_rows) * live_mask
    phase_sh = phase_frac.reshape(N_SRC, shard_rows)
    source_sh = source_index.reshape(N_SRC, shard_rows)
    knot_sh = knot_index.reshape(N_SRC, shard_rows) + jnp.tile(bucket * KNOT_DEV, N_CCD)[None, :]

    def source_step(scan_items):
        design_rows, observed_rows, weight_rows, source_rows, live_rows = scan_items
        moments = jax.ops.segment_sum(row_moments(design_rows, observed_rows, weight_rows).T, source_rows, num_segments=SRC_DEV).T
        params = solve_small(moments)
        fitted = lax.optimization_barrier(jnp.sum(design_rows * jnp.take(params, source_rows, axis=1), 0))
        return (params, live_rows * (observed_rows - fitted))
    params_sh, resid_sh = lax.map(source_step, (design_sh, observed_sh, weight_sh, source_sh, live_mask))
    source_params = params_sh.transpose(1, 0, 2).reshape(5, N_SRC * SRC_DEV)
    zero_knots = jnp.zeros((3, KNOTS + 3), jnp.float32)

    def assemble_step(carried, scan_items):
        factor_rows, weight_rows, phase_rows, knot_rows, resid_rows = scan_items
        spline_terms = spline_basis(phase_rows)
        rhs_part = spread_ref(weight_rows * factor_rows * resid_rows, spline_terms, knot_rows)
        diag_part = spread_ref(weight_rows * factor_rows * factor_rows, [t * t for t in spline_terms], knot_rows)
        return ((carried[0] + rhs_part, carried[1] + diag_part), None)
    (rhs_full, diag_full), _ = lax.scan(assemble_step, (zero_knots, zero_knots), (factor_sh, weight_sh, phase_sh, knot_sh, resid_sh))
    rhs_knots = rhs_full[:, :KNOTS]
    diag_knots = att_ridge + diag_full[:, :KNOTS]
    coefficients = relax_step * rhs_knots / diag_knots
    for iteration in range(1, ITERS):
        padded = jnp.pad(coefficients, ((0, 0), (0, 3)))

        def normal_step(carried, scan_items):
            factor_rows, weight_rows, phase_rows, knot_rows = scan_items
            spline_terms = spline_basis(phase_rows)
            predicted = predict_ref(padded, spline_terms, factor_rows, knot_rows)
            return (carried + spread_ref(weight_rows * factor_rows * predicted, spline_terms, knot_rows), None)
        back_full, _ = lax.scan(normal_step, zero_knots, (factor_sh, weight_sh, phase_sh, knot_sh))
        normal_prod = att_ridge * coefficients + back_full[:, :KNOTS]
        coefficients = coefficients + relax_step * (rhs_knots - normal_prod) / diag_knots
    padded = jnp.pad(coefficients, ((0, 0), (0, 3)))

    def final_step(scan_items):
        factor_rows, phase_rows, knot_rows, resid_rows, live_rows = scan_items
        predicted = predict_ref(padded, spline_basis(phase_rows), factor_rows, knot_rows)
        return live_rows * (resid_rows - predicted)
    residual = lax.map(final_step, (factor_sh, phase_sh, knot_sh, resid_sh, live_mask))
    return (source_params, coefficients, residual.reshape(ROWS))
```

```python
import functools

import jax
import jax.numpy as jnp
from jax import lax
from jax.experimental import pallas as pl
from jax.experimental.pallas import tpu as pltpu
from jax.sharding import PartitionSpec as P

F32 = jnp.float32
BF16 = jnp.bfloat16
MESH = pl.DeviceIdType.MESH
SRC_RIDGE = 1.0
ATT_RIDGE = 1.0
RELAX = 0.15
SWEEPS = 3
BLOCKS = 64
TILES = 65
HALF = 33
KNOTS = 8192
HALO = 6
PAIRS = [(0, 0), (0, 1), (0, 2), (1, 1), (1, 2), (2, 2)]
NT = (((1,), (1,)), ((), ()))
NN = (((1,), (0,)), ((), ()))


def moment_row(m, n):
    m, n = min(m, n), max(m, n)
    return {0: n, 4: n + 2, 1: 7 + n, 3: 10 + n, 2: 14 + n}[m]


def parts(value, count):
    out = []
    rest = value
    for _ in range(count - 1):
        top = rest.astype(BF16).astype(F32)
        out.append(top)
        rest = rest - top
    out.append(rest)
    return out


def solve_rows(row):
    factor = {}
    inverse = {}
    for j in range(5):
        for i in range(j, 5):
            running = row(moment_row(j, i)) + (SRC_RIDGE if i == j else 0.0)
            for k in range(j):
                running = running - factor[i, k] * factor[j, k]
            if i == j:
                inverse[j] = 1.0 / jnp.sqrt(running)
            else:
                factor[i, j] = running * inverse[j]
    forward = []
    for i in range(5):
        running = row(moment_row(i, 5))
        for k in range(i):
            running = running - factor[i, k] * forward[k]
        forward.append(running * inverse[i])
    solved = [None] * 5
    for i in reversed(range(5)):
        running = forward[i]
        for k in range(i + 1, 5):
            running = running - factor[k, i] * solved[k]
        solved[i] = running * inverse[i]
    return solved


def kernel(
    design, obs, wt, ph, ax, sidx, kidx, cnt,
    params_o, att_o, res_o,
    otlo, otk, bb, wl, ax8, lhs, acc, mom, momr, par,
    nloc, nhalf, nsum, nr, npc, nz, nf,
    rloc, rhalf, rsum, rr, rpc, rz, cp, cb, resid,
    ma_s, ma_r, pa_s, pa_r, nh_s, nh_r, np_s, np_r, nz_s, nz_r, ng_s, ng_r,
    rh_s, rh_r, rp_s, rp_r, rz_s, rz_r, cg_s, cg_r,
):
    src = lax.axis_index("src")
    ccd = lax.axis_index("ccd")
    z, y = src // 4, src % 4
    x, core = ccd // 2, ccd % 2
    chip = y * 4 + x
    pid = core * 16 + chip

    def plane(ky, kx, kc):
        return z * 4 + (y + ky) % 4, ((x + kx) % 4) * 2 + (core + kc) % 2

    def along(kz):
        return ((z + kz) % 16) * 4 + y, ccd

    steps16 = [(ky, kx) for ky in range(4) for kx in range(4) if (ky, kx) != (0, 0)]
    steps32 = [(ky, kx, kc) for ky in range(4) for kx in range(4) for kc in range(2) if (ky, kx, kc) != (0, 0, 0)]
    zsteps = [8, 7, 9, 6, 10, 5, 11, 4, 12, 3, 13, 2, 14, 1, 15]
    started = []

    def send(a, b, ssem, rsem, to):
        copy = pltpu.make_async_remote_copy(
            src_ref=a, dst_ref=b, send_sem=ssem, recv_sem=rsem, device_id=to, device_id_type=MESH
        )
        copy.start()
        started.append(copy)
        return copy

    barrier = pltpu.get_barrier_semaphore()
    for k in steps32:
        pl.semaphore_signal(barrier, inc=1, device_id=plane(*k), device_id_type=MESH)
    for k in zsteps:
        pl.semaphore_signal(barrier, inc=1, device_id=along(k), device_id_type=MESH)

    lane = lax.broadcasted_iota(jnp.int32, (8, 128), 1)
    lane1 = lax.broadcasted_iota(jnp.int32, (1, 128), 1)
    sub = lax.broadcasted_iota(jnp.int32, (8, 128), 0)
    iota256 = lax.broadcasted_iota(jnp.int32, (256, 128), 0)
    iota128 = lax.broadcasted_iota(jnp.int32, (128, 128), 0)

    def cols(d):
        return pl.ds(pl.multiple_of(d * 128, 128), 128)

    acc[...] = jnp.zeros_like(acc)

    def moments_step(t, carry):
        for b in range(8):
            d = t * 8 + b
            s_row = sidx[pl.ds(d, 1), :]
            low = s_row & 255
            high = jnp.broadcast_to(s_row >> 8, (72, 128))
            otlo[:, cols(d)] = jnp.where(iota256 == low, 1.0, 0.0).astype(BF16)
            w = jnp.where(lane1 < cnt[0, d], wt[pl.ds(d, 1), :], 0.0)
            wl[pl.ds(d, 1), :] = w
            e = design[:, cols(d)]
            o = obs[pl.ds(d, 1), :]
            ea = jnp.concatenate([e, o, e[4:5], o], 0)
            eb = jnp.concatenate([e[1:5], o, e[3:5], o], 0)
            ec = jnp.concatenate([e[2:5], o, e[2:5], o], 0)
            g = jnp.concatenate(
                [
                    ea * jnp.where(sub < 6, e[0:1] * w, e[4:5] * w),
                    eb * jnp.where(sub < 5, e[1:2] * w, e[3:4] * w),
                    ec * (e[2:3] * w),
                ],
                0,
            )
            stacked = jnp.concatenate(parts(g, 3), 0)
            masked = [jnp.where(high == h, stacked, 0.0) for h in range(4)]
            lhs[:, b * 128 : (b + 1) * 128] = jnp.concatenate(masked, 0).astype(BF16)
        window = otlo[:, pl.ds(pl.multiple_of(t * 1024, 1024), 1024)]
        acc[...] += lax.dot_general(lhs[...], window, NT, preferred_element_type=F32)
        return carry

    lax.fori_loop(0, 8, moments_step, 0)
    for h in range(4):
        total = acc[72 * h : 72 * h + 24] + acc[72 * h + 24 : 72 * h + 48] + acc[72 * h + 48 : 72 * h + 72]
        mom[2 * h] = total[:, :128]
        mom[2 * h + 1] = total[:, 128:]

    pl.semaphore_wait(barrier, len(steps32) + len(zsteps))
    mom_copies = []
    for k in range(1, 8):
        to = (ccd + k) % 8
        mom_copies.append(send(mom.at[to], momr.at[k - 1], ma_s.at[k - 1], ma_r.at[k - 1], (src, to)))

    u = ph[...]
    rem = 1.0 - u
    sq = u * u
    cu = sq * u
    basis = [
        rem * rem * rem / 6.0,
        (3.0 * cu - 6.0 * sq + 4.0) / 6.0,
        (-3.0 * cu + 3.0 * sq + 3.0 * u + 1.0) / 6.0,
        cu / 6.0,
    ]
    bbid = {}
    for i in range(4):
        bb[i] = basis[i]
    for i in range(4):
        for j in range(i, 4):
            bbid[i, j] = 4 + len(bbid)
            bb[bbid[i, j]] = basis[i] * basis[j]
    ax8[0:3, :] = ax[...]
    ax8[3:4, :] = jnp.zeros((1, KNOTS), F32)
    ax8[4:7, :] = ax[...]
    ax8[7:8, :] = jnp.zeros((1, KNOTS), F32)

    lane24 = lax.broadcasted_iota(jnp.int32, (24, 128), 1)

    def spread_shift(value, shift):
        lanes = lax.broadcasted_iota(jnp.int32, value.shape, 1)
        turned = pltpu.roll(value, shift, 1)
        return jnp.where(lanes >= shift, turned, 0.0), jnp.where(lanes < shift, turned, 0.0)

    def normal_step(t, carry):
        for b in range(8):
            d = t * 8 + b
            hot = jnp.where(iota128 == kidx[pl.ds(d, 1), :], 1.0, 0.0).astype(BF16)
            otk[d] = hot
            w = wl[pl.ds(d, 1), :]
            a = [jnp.broadcast_to(ax[i : i + 1, cols(d)], (8, 128)) for i in range(3)]
            wa = [w * a[i] for i in range(3)]
            left = jnp.where(sub < 3, wa[0], jnp.where(sub < 5, wa[1], wa[2]))
            right = jnp.where(
                sub == 0, a[0], jnp.where((sub == 1) | (sub == 3), a[1], a[2])
            )
            base = left * right
            tails = [
                jnp.where(sub == 6, wa[0] * a[0], wa[0] * a[1]),
                jnp.where(sub == 6, wa[0] * a[2], wa[1] * a[1]),
                jnp.where(sub == 6, wa[1] * a[2], wa[2] * a[2]),
            ]

            def term(i, j):
                return bb[bbid[i, j], pl.ds(d, 1), :]

            only = jnp.where(sub < 6, base, 0.0)
            groups = [jnp.where(sub < 6, base * term(0, o), tails[o] * term(0, 3)) for o in range(3)]
            groups += [only * term(1, 1), only * term(1, 2), only * term(1, 3)]
            groups += [only * term(2, 2), only * term(2, 3), only * term(3, 3)]
            stacked = jnp.concatenate(groups, 0)
            both = jnp.concatenate(parts(stacked, 2), 0).astype(BF16)
            sums = lax.dot_general(both, hot, NT, preferred_element_type=F32)
            sums = sums[:72] + sums[72:]
            c0, v0 = spread_shift(sums[0:24], HALO)
            c1, v1 = spread_shift(sums[24:48], HALO + 1)
            c2, v2 = spread_shift(sums[48:64], HALO + 2)
            c3, v3 = spread_shift(sums[64:72], HALO + 3)
            zeros8 = jnp.zeros((8, 128), F32)
            zeros16 = jnp.zeros((16, 128), F32)
            here = c0 + c1 + jnp.concatenate([c2, zeros8], 0) + jnp.concatenate([c3, zeros16], 0)
            nloc[d] = here + carry
            carry = v0 + v1 + jnp.concatenate([v2, zeros8], 0) + jnp.concatenate([v3, zeros16], 0)
        return carry

    nloc[BLOCKS] = lax.fori_loop(0, 8, normal_step, jnp.zeros((24, 128), F32))
    mate = (src, x * 2 + (core + 1) % 2)
    nhalf_copy = send(nloc.at[pl.ds(32 * ((core + 1) % 2), HALF)], nhalf, nh_s, nh_r, mate)

    for copy in mom_copies:
        copy.wait_recv()
    whole = mom[ccd]
    for k in range(7):
        whole = whole + momr[k]
    solved = solve_rows(lambda r: whole[r : r + 1])
    par[ccd] = jnp.concatenate(solved + [jnp.zeros((3, 128), F32)], 0)
    for k in range(1, 8):
        send(par.at[ccd], par.at[ccd], pa_s.at[k - 1], pa_r.at[k - 1], (src, (ccd + k) % 8))

    nhalf_copy.wait_recv()
    for i in range(HALF):
        nsum[i] = nloc[32 * core + i] + nhalf[i]
    n_copies = []
    for i, (ky, kx) in enumerate(steps16):
        there = ((y + ky) % 4) * 4 + (x + kx) % 4
        n_copies.append(send(nsum.at[pl.ds(2 * there, 3)], nr.at[i], np_s.at[i], np_r.at[i], plane(ky, kx, 0)))

    for k in range(1, 8):
        sender = (ccd + 8 - k) % 8
        pltpu.make_async_remote_copy(
            src_ref=par.at[sender], dst_ref=par.at[sender], send_sem=pa_s.at[k - 1], recv_sem=pa_r.at[k - 1],
            device_id=(src, sender), device_id_type=MESH,
        ).wait_recv()
    for c in range(8):
        params_o[:, c * 128 : (c + 1) * 128] = par[c, 0:5]
    table = jnp.concatenate([jnp.concatenate([par[2 * h], par[2 * h + 1]], 1) for h in range(4)], 0)
    table = jnp.concatenate(parts(table, 3), 0).astype(BF16)

    def residual_step(t, carry):
        window = otlo[:, pl.ds(pl.multiple_of(t * 1024, 1024), 1024)]
        picked = lax.dot_general(table, window, NN, preferred_element_type=F32)
        picked = picked[0:32] + picked[32:64] + picked[64:96]
        for b in range(8):
            d = t * 8 + b
            high = jnp.broadcast_to(sidx[pl.ds(d, 1), :] >> 8, (8, 128))
            own = picked[:, b * 128 : (b + 1) * 128]
            chosen = own[0:8]
            for h in range(1, 4):
                chosen = jnp.where(high == h, own[8 * h : 8 * h + 8], chosen)
            fitted = jnp.sum(chosen[0:5] * design[:, cols(d)], 0, keepdims=True)
            r = jnp.where(lane1 < cnt[0, d], obs[pl.ds(d, 1), :] - fitted, 0.0)
            resid[pl.ds(d, 1), :] = r
            wr = wl[pl.ds(d, 1), :] * r
            a = ax8[:, cols(d)]
            upper = sub < 4
            pair01 = a * jnp.where(upper, wr * bb[0, pl.ds(d, 1), :], wr * bb[1, pl.ds(d, 1), :])
            pair23 = a * jnp.where(upper, wr * bb[2, pl.ds(d, 1), :], wr * bb[3, pl.ds(d, 1), :])
            stacked = jnp.concatenate([pair01, pair23], 0)
            split = jnp.concatenate(parts(stacked, 3), 0).astype(BF16)
            sums = lax.dot_general(split, otk[d], NT, preferred_element_type=F32)
            sums = sums[0:16] + sums[16:32] + sums[32:48]
            here = carry
            over = jnp.zeros((8, 128), F32)
            for g in range(2):
                value = sums[8 * g : 8 * g + 8]
                first, second = HALO + 2 * g, HALO + 2 * g + 1
                turned = jnp.where(upper, pltpu.roll(value, first, 1), pltpu.roll(value, second, 1))
                limit = jnp.where(upper, first, second)
                here = here + jnp.where(lane >= limit, turned, 0.0)
                over = over + jnp.where(lane < limit, turned, 0.0)
            folded = here + pltpu.roll(here, 4, 0)
            rloc[d] = folded[0:4]
            carry = over
        return carry

    last = lax.fori_loop(0, 8, residual_step, jnp.zeros((8, 128), F32))
    last = last + pltpu.roll(last, 4, 0)
    rloc[BLOCKS] = last[0:4]

    rhalf_copy = send(rloc.at[pl.ds(32 * ((core + 1) % 2), HALF)], rhalf, rh_s, rh_r, mate)
    rhalf_copy.wait_recv()
    for i in range(HALF):
        rsum[i] = rloc[32 * core + i] + rhalf[i]
    r_copies = []
    for i, (ky, kx) in enumerate(steps16):
        there = ((y + ky) % 4) * 4 + (x + kx) % 4
        r_copies.append(send(rsum.at[pl.ds(2 * there, 3)], rr.at[i], rp_s.at[i], rp_r.at[i], plane(ky, kx, 0)))

    for copy in n_copies:
        copy.wait_recv()
    for t in range(3):
        total = nsum[2 * chip + t]
        for i in range(15):
            total = total + nr[i, t]
        for g in range(3):
            npc[3 * t + g] = total[8 * g : 8 * g + 8]
    owners = [(16 * g) // 9 for g in range(9)]
    mine = (9 * z + 15) // 16
    is_owner = (16 * mine) // 9 == z
    for g, owner in enumerate(owners):
        step = (owner + 16 - z) % 16

        @pl.when(owner != z)
        def _(g=g, owner=owner, step=step):
            pltpu.make_async_remote_copy(
                src_ref=npc.at[g], dst_ref=nz.at[step - 1], send_sem=nz_s.at[g], recv_sem=nz_r.at[step - 1],
                device_id=(owner * 4 + y, ccd), device_id_type=MESH,
            ).start()

    for copy in r_copies:
        copy.wait_recv()
    for t in range(3):
        total = rsum[2 * chip + t]
        for i in range(15):
            total = total + rr[i, t]
        rpc[t] = total
    rz_copies = []
    for kz in zsteps:
        rz_copies.append(send(rpc, rz.at[kz - 1], rz_s.at[kz - 1], rz_r.at[kz - 1], along(kz)))

    @pl.when(is_owner)
    def _():
        total = npc[mine]
        for k in range(15):
            pltpu.make_async_remote_copy(
                src_ref=npc.at[0], dst_ref=nz.at[k], send_sem=nz_s.at[0], recv_sem=nz_r.at[k],
                device_id=along(k + 1), device_id_type=MESH,
            ).wait_recv()
            total = total + nz[k]
        nf[mine] = total
        for k in zsteps:
            pltpu.make_async_remote_copy(
                src_ref=nf.at[mine], dst_ref=nf.at[mine], send_sem=ng_s.at[k - 1], recv_sem=ng_r.at[mine],
                device_id=along(k), device_id_type=MESH,
            ).start()

    for copy in rz_copies:
        copy.wait_recv()
    rows = []
    for t in range(3):
        total = rpc[t]
        for i in range(15):
            total = total + rz[i, t]
        rows.append(total)
    rhs4 = jnp.concatenate(rows, 1)
    for g, owner in enumerate(owners):

        @pl.when(owner != z)
        def _(g=g, owner=owner):
            pltpu.make_async_remote_copy(
                src_ref=nf.at[g], dst_ref=nf.at[g], send_sem=ng_s.at[0], recv_sem=ng_r.at[g],
                device_id=(owner * 4 + y, ccd), device_id_type=MESH,
            ).wait_recv()

    def wide(row):
        return jnp.broadcast_to(row, (8, 384))

    def band(o, pair):
        g, s = (o, pair) if o < 3 else (pair // 2, 6 + pair % 2)
        return wide(jnp.concatenate([nf[3 * t + g, s : s + 1] for t in range(3)], 1))

    bands = [{} for _ in range(4)]
    for o in range(4):
        for p, (a, b) in enumerate(PAIRS):
            bands[o][a, b] = bands[o][b, a] = band(o, p)
    inside = lax.broadcasted_iota(jnp.int32, (8, 384), 1) < KNOTS + HALO - 256 * pid
    rhs = [wide(rhs4[i : i + 1]) for i in range(3)]
    scale = [RELAX / (ATT_RIDGE + bands[0][i, i]) for i in range(3)]
    coef = [jnp.where(inside, rhs[i] * scale[i], 0.0) for i in range(3)]
    for _ in range(1, SWEEPS):
        ahead = [[pltpu.roll(coef[i], 384 - o, 1) for i in range(3)] for o in range(1, 4)]
        fresh = []
        for i in range(3):
            product = coef[i] * ATT_RIDGE
            for k in range(3):
                product = product + bands[0][i, k] * coef[k]
            for o in range(1, 4):
                back = bands[o][i, 0] * coef[0] + bands[o][i, 1] * coef[1] + bands[o][i, 2] * coef[2]
                product = product + pltpu.roll(back, o, 1)
                for k in range(3):
                    product = product + bands[o][i, k] * ahead[o - 1][k]
            fresh.append(jnp.where(inside, coef[i] + scale[i] * (rhs[i] - product), 0.0))
        coef = fresh
    cp[:, 3:4, :] = jnp.zeros((2, 1, 128), F32)
    for i in range(3):
        moved = pltpu.roll(coef[i], 384 - HALO, 1)
        for t in range(2):
            cp[t, i : i + 1] = moved[0:1, t * 128 : (t + 1) * 128]
    for t in range(2):
        cb[2 * pid + t] = cp[t]
    cb[BLOCKS] = jnp.zeros((4, 128), F32)
    for i, k in enumerate(steps32):
        send(cp, cb.at[pl.ds(2 * pid, 2)], cg_s.at[i], cg_r.at[i], plane(*k))
    for i, (ky, kx, kc) in enumerate(steps32):
        sy, sx, sc = (y + 4 - ky) % 4, (x + 4 - kx) % 4, (core + 2 - kc) % 2
        slot = cb.at[pl.ds(2 * (sc * 16 + sy * 4 + sx), 2)]
        pltpu.make_async_remote_copy(
            src_ref=cp, dst_ref=slot, send_sem=cg_s.at[i], recv_sem=cg_r.at[i],
            device_id=(z * 4 + sy, sx * 2 + sc), device_id_type=MESH,
        ).wait_recv()
    att_o[...] = cb[src][0:3]

    def final_step(t, carry):
        for b in range(8):
            d = t * 8 + b
            now = jnp.concatenate([cb[d], cb[d + 1]], 0)
            shifted = []
            for j in range(4):
                turned = now if j == 0 else pltpu.roll(now, 128 - j, 1)
                up = pltpu.roll(turned, 4, 0)
                shifted.append(jnp.where(lane < 128 - j, turned, up))
            pair01 = jnp.where(sub < 4, shifted[0], pltpu.roll(shifted[1], 4, 0))
            pair23 = jnp.where(sub < 4, shifted[2], pltpu.roll(shifted[3], 4, 0))
            stacked = jnp.concatenate([pair01, pair23], 0)
            split = jnp.concatenate(parts(stacked, 3), 0).astype(BF16)
            picked = lax.dot_general(split, otk[d], NN, preferred_element_type=F32)
            picked = picked[0:16] + picked[16:32] + picked[32:48]
            upper = sub < 4
            b01 = jnp.where(upper, bb[0, pl.ds(d, 1), :], bb[1, pl.ds(d, 1), :])
            b23 = jnp.where(upper, bb[2, pl.ds(d, 1), :], bb[3, pl.ds(d, 1), :])
            terms = ax8[:, cols(d)] * (picked[0:8] * b01 + picked[8:16] * b23)
            predicted = jnp.sum(terms, 0, keepdims=True)
            res_o[pl.ds(d, 1), :] = jnp.where(
                lane1 < cnt[0, d], resid[pl.ds(d, 1), :] - predicted, 0.0
            )
        return carry

    lax.fori_loop(0, 8, final_step, 0)

    for copy in started:
        copy.wait_send()
    for g, owner in enumerate(owners):

        @pl.when(owner != z)
        def _(g=g, owner=owner):
            pltpu.make_async_remote_copy(
                src_ref=npc.at[g], dst_ref=nz.at[0], send_sem=nz_s.at[g], recv_sem=nz_r.at[0],
                device_id=(owner * 4 + y, ccd), device_id_type=MESH,
            ).wait_send()

    @pl.when(is_owner)
    def _():
        for k in zsteps:
            pltpu.make_async_remote_copy(
                src_ref=nf.at[mine], dst_ref=nf.at[mine], send_sem=ng_s.at[k - 1], recv_sem=ng_r.at[mine],
                device_id=along(k), device_id_type=MESH,
            ).wait_send()


def on_device(design, observed, weight, phase_frac, axis_factors, source_index, knot_index, counts):
    dma = pltpu.SemaphoreType.DMA
    vm = lambda *shape: pltpu.VMEM(shape, F32)
    vmem = pl.BlockSpec(memory_space=pltpu.VMEM)
    square = lambda v: v.reshape(64, 128)
    params, attitude, residual = pl.pallas_call(
        kernel,
        out_shape=(
            jax.ShapeDtypeStruct((5, 1024), F32),
            jax.ShapeDtypeStruct((3, 128), F32),
            jax.ShapeDtypeStruct((64, 128), F32),
        ),
        in_specs=[vmem] * 7 + [pl.BlockSpec(memory_space=pltpu.SMEM)],
        out_specs=(vmem, vmem, vmem),
        scratch_shapes=[
            pltpu.VMEM((256, 8192), BF16),
            pltpu.VMEM((64, 128, 128), BF16),
            vm(14, 64, 128), vm(64, 128), vm(8, 8192),
            pltpu.VMEM((288, 1024), BF16),
            vm(288, 256), vm(8, 24, 128), vm(7, 24, 128), vm(8, 8, 128),
            vm(TILES, 24, 128), vm(HALF, 24, 128), vm(HALF, 24, 128), vm(15, 3, 24, 128),
            vm(9, 8, 128), vm(15, 8, 128), vm(9, 8, 128),
            vm(TILES, 4, 128), vm(HALF, 4, 128), vm(HALF, 4, 128), vm(15, 3, 4, 128),
            vm(3, 4, 128), vm(15, 3, 4, 128), vm(2, 4, 128), vm(TILES, 4, 128), vm(64, 128),
            dma((7,)), dma((7,)), dma((7,)), dma((7,)),
            dma, dma, dma((15,)), dma((15,)), dma((9,)), dma((15,)), dma((15,)), dma((9,)),
            dma, dma, dma((15,)), dma((15,)), dma((15,)), dma((15,)), dma((31,)), dma((31,)),
        ],
        compiler_params=pltpu.CompilerParams(
            collective_id=0, has_side_effects=True, vmem_limit_bytes=48 * 1024 * 1024
        ),
    )(
        design, square(observed), square(weight), square(phase_frac), axis_factors,
        square(source_index), square(knot_index), counts.reshape(1, 64),
    )
    return params, attitude, residual.reshape(8192)


def solution(mesh):
    rows = P(("src", "ccd"))
    wide = P(None, ("src", "ccd"))
    in_specs = (wide, rows, rows, rows, wide, rows, rows, P("src", "ccd", None))
    out_specs = (P(None, "src"), P(None, "src"), rows)
    return jax.shard_map(on_device, mesh=mesh, in_specs=in_specs, out_specs=out_specs, check_vma=False)
```

```python
import functools

import jax
import jax.numpy as jnp
from jax import lax
from jax.experimental import pallas as pl
from jax.experimental.pallas import tpu as pltpu
from jax.sharding import PartitionSpec as P

F32 = jnp.float32
BF16 = jnp.bfloat16
MESH = pl.DeviceIdType.MESH
SRC_RIDGE = 1.0
ATT_RIDGE = 1.0
RELAX = 0.15
SWEEPS = 3
BLOCKS = 64
TILES = 65
HALF = 33
KNOTS = 8192
HALO = 6
UNROLL = 16
PAIRS = [(0, 0), (0, 1), (0, 2), (1, 1), (1, 2), (2, 2)]
NT = (((1,), (1,)), ((), ()))
NN = (((1,), (0,)), ((), ()))


def moment_row(m, n):
    m, n = min(m, n), max(m, n)
    return {0: n, 4: n + 2, 1: 7 + n, 3: 10 + n, 2: 14 + n}[m]


def parts(value, count):
    out = []
    rest = value
    for _ in range(count - 1):
        top = rest.astype(BF16).astype(F32)
        out.append(top)
        rest = rest - top
    out.append(rest)
    return out


def solve_rows(row):
    factor = {}
    inverse = {}
    for j in range(5):
        for i in range(j, 5):
            running = row(moment_row(j, i)) + (SRC_RIDGE if i == j else 0.0)
            for k in range(j):
                running = running - factor[i, k] * factor[j, k]
            if i == j:
                inverse[j] = 1.0 / jnp.sqrt(running)
            else:
                factor[i, j] = running * inverse[j]
    forward = []
    for i in range(5):
        running = row(moment_row(i, 5))
        for k in range(i):
            running = running - factor[i, k] * forward[k]
        forward.append(running * inverse[i])
    solved = [None] * 5
    for i in reversed(range(5)):
        running = forward[i]
        for k in range(i + 1, 5):
            running = running - factor[k, i] * solved[k]
        solved[i] = running * inverse[i]
    return solved


def kernel(
    design_h, obs_h, wt_h, ph_h, ax_h, sidx_h, kidx_h, cnt_h,
    params_h, att_h, res_h,
    params_o, att_o, res_o, out_sem,
    design, obs, wt, ph, ax, sidx, kidx, cnt, in_sem,
    otlo, otk, bb, wl, ax8, lhs, acc, mom, momr, par,
    nloc, nhalf, nsum, nr, npc, nz, nf,
    rloc, rhalf, rsum, rr, rpc, rz, cp, cb, resid,
    ma_s, ma_r, pa_s, pa_r, nh_s, nh_r, np_s, np_r, nz_s, nz_r, ng_s, ng_r,
    rh_s, rh_r, rp_s, rp_r, rz_s, rz_r, cg_s, cg_r,
):
    src = lax.axis_index("src")
    ccd = lax.axis_index("ccd")
    z, y = src // 4, src % 4
    x, core = ccd // 2, ccd % 2
    chip = y * 4 + x
    pid = core * 16 + chip

    def plane(ky, kx, kc):
        return z * 4 + (y + ky) % 4, ((x + kx) % 4) * 2 + (core + kc) % 2

    def along(kz):
        return ((z + kz) % 16) * 4 + y, ccd

    steps16 = [(2, 2), (2, 1), (2, 3), (1, 2), (3, 2), (2, 0), (0, 2), (1, 1), (3, 3), (1, 3), (3, 1), (1, 0), (3, 0), (0, 1), (0, 3)]
    steps32 = [(ky, kx, kc) for ky, kx in steps16 for kc in (1, 0)] + [(0, 0, 1)]
    zsteps = [8, 7, 9, 6, 10, 5, 11, 4, 12, 3, 13, 2, 14, 1, 15]
    started = []

    loads = []
    held = (sidx, wt, design, obs, ph, ax, kidx)
    for i, (a, b) in enumerate(zip((sidx_h, wt_h, design_h, obs_h, ph_h, ax_h, kidx_h), held)):
        loads.append(pltpu.make_async_copy(a, b, in_sem.at[i]))
        loads[-1].start()

    loads.insert(0, pltpu.make_async_copy(cnt_h, cnt, in_sem.at[7]))
    loads[0].start()

    def send(a, b, ssem, rsem, to):
        copy = pltpu.make_async_remote_copy(
            src_ref=a, dst_ref=b, send_sem=ssem, recv_sem=rsem, device_id=to, device_id_type=MESH
        )
        copy.start()
        started.append(copy)
        return copy

    barrier = pltpu.get_barrier_semaphore()
    for k in steps32:
        pl.semaphore_signal(barrier, inc=1, device_id=plane(*k), device_id_type=MESH)
    for k in zsteps:
        pl.semaphore_signal(barrier, inc=1, device_id=along(k), device_id_type=MESH)

    lane = lax.broadcasted_iota(jnp.int32, (8, 128), 1)
    lane1 = lax.broadcasted_iota(jnp.int32, (1, 128), 1)
    sub = lax.broadcasted_iota(jnp.int32, (8, 128), 0)
    iota256 = lax.broadcasted_iota(jnp.int32, (256, 128), 0).astype(F32).astype(BF16)
    one, zero = jnp.ones((256, 128), BF16), jnp.zeros((256, 128), BF16)
    nought = jnp.zeros((64, 128), BF16)

    def cols(d):
        return pl.ds(pl.multiple_of(d * 128, 128), 128)

    def tall(row, count):
        packed = jnp.broadcast_to(row.astype(F32), (16, 128)).astype(BF16)
        return jnp.concatenate([packed] * count, 0)

    def hot(row):
        return jnp.where(iota256 == tall(row, 16), one, zero)

    for copy in loads[:5]:
        copy.wait()
    acc[...] = jnp.zeros_like(acc)

    def moments_step(t, carry):
        total = None
        for part in range(UNROLL // 8):
            for b in range(8):
                d = t * UNROLL + part * 8 + b
                s_row = sidx[pl.ds(d, 1), :]
                otlo[:, cols(d)] = hot(s_row & 255)
                high = tall(s_row >> 8, 4)
                w = jnp.where(lane1 < cnt[0, d], wt[pl.ds(d, 1), :], 0.0)
                wl[pl.ds(d, 1), :] = w
                e = jnp.concatenate([design[:, cols(d)], jnp.zeros((3, 128), F32)], 0)
                o = jnp.broadcast_to(obs[pl.ds(d, 1), :], (8, 128))
                e0, e1, e2, e3, e4 = [design[i : i + 1, cols(d)] for i in range(5)]
                down = pltpu.roll(e, 2, 0)
                ea = jnp.where(sub < 5, e, jnp.where(sub == 6, e4, o))
                eb = jnp.where(sub < 4, pltpu.roll(e, 7, 0), jnp.where((sub == 5) | (sub == 6), down, o))
                ec = jnp.where(sub < 3, pltpu.roll(e, 6, 0), jnp.where((sub > 3) & (sub < 7), down, o))
                ga = parts(w * ea * jnp.where(sub < 6, e0, e4), 3)
                gb = parts(w * eb * jnp.where(sub < 5, e1, e3), 3)
                gc = parts(w * ec * e2, 3)
                rows = [ga[0], gb[0], ga[1], gb[1], ga[2], gb[2], jnp.where(sub < 4, gc[0], gc[1]), gc[2]]
                stacked = jnp.concatenate(rows, 0).astype(BF16)
                for h in range(4):
                    masked = jnp.where(high == jnp.full((64, 128), h, BF16), stacked, nought)
                    lhs[part, 64 * h : 64 * h + 64, b * 128 : b * 128 + 128] = masked
            window = otlo[:, pl.ds(pl.multiple_of(t * UNROLL * 128 + part * 1024, 1024), 1024)]
            product = lax.dot_general(lhs[part], window, NT, preferred_element_type=F32)
            total = product if total is None else total + product
        acc[...] += total
        return carry

    lax.fori_loop(0, BLOCKS // UNROLL, moments_step, 0)
    for h in range(4):
        v = [acc[64 * h + 8 * i : 64 * h + 8 * i + 8] for i in range(8)]
        tail = v[6] + pltpu.roll(v[6], 4, 0) + v[7]
        total = jnp.concatenate([v[0] + v[2] + v[4], v[1] + v[3] + v[5], tail], 0)
        mom[2 * h] = total[:, :128]
        mom[2 * h + 1] = total[:, 128:]
    pl.semaphore_wait(barrier, len(steps32) + len(zsteps))
    mom_copies = []
    for k in (4, 5, 3, 2, 6, 7, 1):
        to = (ccd + k) % 8
        mom_copies.append(send(mom.at[to], momr.at[k - 1], ma_s.at[k - 1], ma_r.at[k - 1], (src, to)))

    for copy in loads[5:]:
        copy.wait()
    u = ph[...]
    rem = 1.0 - u
    sq = u * u
    cu = sq * u
    basis = [
        rem * rem * rem / 6.0,
        (3.0 * cu - 6.0 * sq + 4.0) / 6.0,
        (-3.0 * cu + 3.0 * sq + 3.0 * u + 1.0) / 6.0,
        cu / 6.0,
    ]
    bbid = {}
    for i in range(4):
        bb[i] = basis[i]
    for i in range(4):
        for j in range(i, 4):
            bbid[i, j] = 4 + len(bbid)
            bb[bbid[i, j]] = basis[i] * basis[j]
    ax8[0:3, :] = ax[...]
    ax8[3:4, :] = jnp.zeros((1, KNOTS), F32)
    ax8[4:7, :] = ax[...]
    ax8[7:8, :] = jnp.zeros((1, KNOTS), F32)

    def spread_shift(value, shift):
        lanes = lax.broadcasted_iota(jnp.int32, value.shape, 1)
        turned = pltpu.roll(value, shift, 1)
        return jnp.where(lanes >= shift, turned, 0.0), jnp.where(lanes < shift, turned, 0.0)

    def normal_step(t, carry):
        for pair in range(UNROLL // 2):
            p = t * (UNROLL // 2) + pair
            halves = []
            for b in range(2):
                d = 2 * p + b
                otk[p, :, b * 128 : b * 128 + 128] = hot(kidx[pl.ds(d, 1), :] + 128 * b)
                w = wl[pl.ds(d, 1), :]
                a = [jnp.broadcast_to(ax[i : i + 1, cols(d)], (8, 128)) for i in range(3)]
                wa = [w * a[i] for i in range(3)]
                left = jnp.where(sub < 3, wa[0], jnp.where(sub < 5, wa[1], wa[2]))
                right = jnp.where(sub == 0, a[0], jnp.where((sub == 1) | (sub == 3), a[1], a[2]))
                only = jnp.where(sub < 6, left * right, 0.0)
                tails = [
                    wa[0] * jnp.where(sub == 6, a[0], a[1]),
                    jnp.where(sub == 6, wa[0], wa[1]) * jnp.where(sub == 6, a[2], a[1]),
                    a[2] * jnp.where(sub == 6, wa[1], wa[2]),
                ]

                def term(i, j):
                    return bb[bbid[i, j], pl.ds(d, 1), :]

                last = term(0, 3)
                groups = [jnp.where(sub < 6, only * term(0, o), tails[o] * last) for o in range(3)]
                groups += [only * term(1, 1), only * term(1, 2), only * term(1, 3)]
                groups += [only * term(2, 2), only * term(2, 3), only * term(3, 3)]
                stacked = jnp.concatenate(groups, 0)
                halves.append(jnp.concatenate(parts(stacked, 2), 0).astype(BF16))
            both = jnp.concatenate(halves, 1)
            sums = lax.dot_general(both, otk[p], NT, preferred_element_type=F32)
            sums = sums[:72] + sums[72:]
            zeros8 = jnp.zeros((8, 128), F32)
            zeros16 = jnp.zeros((16, 128), F32)
            for b in range(2):
                own = sums[:, b * 128 : b * 128 + 128]
                c0, v0 = spread_shift(own[0:24], HALO)
                c1, v1 = spread_shift(own[24:48], HALO + 1)
                c2, v2 = spread_shift(own[48:64], HALO + 2)
                c3, v3 = spread_shift(own[64:72], HALO + 3)
                here = c0 + c1 + jnp.concatenate([c2, zeros8], 0) + jnp.concatenate([c3, zeros16], 0)
                nloc[2 * p + b] = here + carry
                carry = v0 + v1 + jnp.concatenate([v2, zeros8], 0) + jnp.concatenate([v3, zeros16], 0)
        return carry

    nloc[BLOCKS] = lax.fori_loop(0, BLOCKS // UNROLL, normal_step, jnp.zeros((24, 128), F32))
    mate = (src, x * 2 + (core + 1) % 2)
    nhalf_copy = send(nloc.at[pl.ds(32 * ((core + 1) % 2), HALF)], nhalf, nh_s, nh_r, mate)

    for copy in mom_copies:
        copy.wait_recv()
    whole = mom[ccd]
    for k in range(7):
        whole = whole + momr[k]
    solved = solve_rows(lambda r: whole[r : r + 1])
    par[ccd] = jnp.concatenate(solved + [jnp.zeros((3, 128), F32)], 0)
    for k in (4, 5, 3, 2, 6, 7, 1):
        send(par.at[ccd], par.at[ccd], pa_s.at[k - 1], pa_r.at[k - 1], (src, (ccd + k) % 8))
    def pack(halo):
        near = jnp.where(lane < 32, pltpu.roll(halo[1], 16, 1), pltpu.roll(halo[2], 32, 1))
        return jnp.where(lane < 16, halo[0], near)

    nhalf_copy.wait_recv()
    for i in range(16):
        for t in range(2):
            tile = nloc[32 * core + 2 * i + t] + nhalf[2 * i + t]
            for g in range(3):
                nsum[i, 3 * t + g] = tile[8 * g : 8 * g + 8]
        if i:
            nsum[i - 1, 6] = pack([nsum[i, g] for g in range(3)])
    tile = nloc[32 * core + 32] + nhalf[32]
    nsum[15, 6] = pack([tile[8 * g : 8 * g + 8] for g in range(3)])

    def to_owner(i):
        ky, kx = steps16[i]
        there = ((y + ky) % 4) * 4 + (x + kx) % 4
        return send(nsum.at[there], nr.at[i], np_s.at[i], np_r.at[i], plane(ky, kx, 0))

    n_copies = [to_owner(i) for i in range(15)]

    for k in range(1, 8):
        sender = (ccd + 8 - k) % 8
        pltpu.make_async_remote_copy(
            src_ref=par.at[sender], dst_ref=par.at[sender], send_sem=pa_s.at[k - 1], recv_sem=pa_r.at[k - 1],
            device_id=(src, sender), device_id_type=MESH,
        ).wait_recv()
    table = jnp.concatenate([jnp.concatenate([par[2 * h], par[2 * h + 1]], 1) for h in range(4)], 0)
    table = jnp.concatenate(parts(table, 3), 0).astype(BF16)
    upper = sub < 4

    def residual_step(t, carry):
        for part in range(UNROLL // 8):
            window = otlo[:, pl.ds(pl.multiple_of(t * UNROLL * 128 + part * 1024, 1024), 1024)]
            picked = lax.dot_general(table, window, NN, preferred_element_type=F32)
            picked = picked[0:32] + picked[32:64] + picked[64:96]
            for pair in range(4):
                halves = []
                p = t * (UNROLL // 2) + part * 4 + pair
                for b in range(2):
                    d = 2 * p + b
                    high = jnp.broadcast_to(sidx[pl.ds(d, 1), :] >> 8, (8, 128))
                    own = picked[:, pair * 256 + b * 128 : pair * 256 + b * 128 + 128]
                    chosen = own[0:8]
                    for h in range(1, 4):
                        chosen = jnp.where(high == h, own[8 * h : 8 * h + 8], chosen)
                    fitted = jnp.sum(chosen[0:5] * design[:, cols(d)], 0, keepdims=True)
                    r = jnp.where(lane1 < cnt[0, d], obs[pl.ds(d, 1), :] - fitted, 0.0)
                    resid[pl.ds(d, 1), :] = r
                    wr = jnp.broadcast_to(wl[pl.ds(d, 1), :] * r, (8, 128))
                    a = ax8[:, cols(d)] * wr
                    pair01 = a * jnp.where(upper, bb[0, pl.ds(d, 1), :], bb[1, pl.ds(d, 1), :])
                    pair23 = a * jnp.where(upper, bb[2, pl.ds(d, 1), :], bb[3, pl.ds(d, 1), :])
                    stacked = jnp.concatenate([pair01, pair23], 0)
                    halves.append(jnp.concatenate(parts(stacked, 3), 0).astype(BF16))
                both = jnp.concatenate(halves, 1)
                sums = lax.dot_general(both, otk[p], NT, preferred_element_type=F32)
                sums = sums[0:16] + sums[16:32] + sums[32:48]
                for b in range(2):
                    here = carry
                    over = jnp.zeros((8, 128), F32)
                    for g in range(2):
                        value = sums[8 * g : 8 * g + 8, b * 128 : b * 128 + 128]
                        first, second = HALO + 2 * g, HALO + 2 * g + 1
                        turned = jnp.where(upper, pltpu.roll(value, first, 1), pltpu.roll(value, second, 1))
                        limit = jnp.where(upper, first, second)
                        here = here + jnp.where(lane >= limit, turned, 0.0)
                        over = over + jnp.where(lane < limit, turned, 0.0)
                    folded = here + pltpu.roll(here, 4, 0)
                    rloc[2 * p + b] = folded[0:4]
                    carry = over
        return carry

    last = lax.fori_loop(0, BLOCKS // UNROLL, residual_step, jnp.zeros((8, 128), F32))
    last = last + pltpu.roll(last, 4, 0)
    rloc[BLOCKS] = last[0:4]

    rhalf_copy = send(rloc.at[pl.ds(32 * ((core + 1) % 2), HALF)], rhalf, rh_s, rh_r, mate)
    for c in range(8):
        params_o[:, c * 128 : (c + 1) * 128] = par[c, 0:5]
    params_out = pltpu.make_async_copy(params_o, params_h, out_sem.at[0])
    params_out.start()
    rhalf_copy.wait_recv()
    for i in range(16):
        for t in range(2):
            rsum[i, t] = rloc[32 * core + 2 * i + t] + rhalf[2 * i + t]
        rsum[i, 2] = rloc[32 * core + 2 * i + 2] + rhalf[2 * i + 2]
    r_copies = []
    for i, (ky, kx) in enumerate(steps16):
        there = ((y + ky) % 4) * 4 + (x + kx) % 4
        r_copies.append(send(rsum.at[there], rr.at[i], rp_s.at[i], rp_r.at[i], plane(ky, kx, 0)))

    for copy in n_copies:
        copy.wait_recv()
    for g in range(7):
        total = nsum[chip, g]
        for i in range(15):
            total = total + nr[i, g]
        npc[g] = total
    owners = [(16 * g) // 7 for g in range(7)]
    mine = (7 * z + 15) // 16
    is_owner = (16 * mine) // 7 == z
    for g, owner in enumerate(owners):
        step = (owner + 16 - z) % 16

        @pl.when(owner != z)
        def _(g=g, owner=owner, step=step):
            pltpu.make_async_remote_copy(
                src_ref=npc.at[g], dst_ref=nz.at[step - 1], send_sem=nz_s.at[g], recv_sem=nz_r.at[step - 1],
                device_id=(owner * 4 + y, ccd), device_id_type=MESH,
            ).start()

    for copy in r_copies:
        copy.wait_recv()
    rows = []
    for t in range(3):
        total = rsum[chip, t]
        for i in range(15):
            total = total + rr[i, t]
        rows.append(total)
    low = jnp.concatenate(rows[:2], 0)
    edge = jnp.where(lane1 < 16, rows[2][0:1], jnp.where(lane1 < 32, pltpu.roll(rows[2], 16, 1)[1:2], pltpu.roll(rows[2], 32, 1)[2:3]))
    rpc[...] = jnp.where((sub == 3) | (sub == 7), jnp.broadcast_to(edge, (8, 128)), low)
    rz_copies = []
    for kz in zsteps:
        rz_copies.append(send(rpc, rz.at[kz - 1], rz_s.at[kz - 1], rz_r.at[kz - 1], along(kz)))

    @pl.when(is_owner)
    def _():
        total = npc[mine]
        for k in range(15):
            pltpu.make_async_remote_copy(
                src_ref=npc.at[0], dst_ref=nz.at[k], send_sem=nz_s.at[0], recv_sem=nz_r.at[k],
                device_id=along(k + 1), device_id_type=MESH,
            ).wait_recv()
            total = total + nz[k]
        nf[mine] = total
        for k in zsteps:
            pltpu.make_async_remote_copy(
                src_ref=nf.at[mine], dst_ref=nf.at[mine], send_sem=ng_s.at[k - 1], recv_sem=ng_r.at[mine],
                device_id=along(k), device_id_type=MESH,
            ).start()

    for copy in rz_copies:
        copy.wait_recv()
    flat = rpc[...]
    for i in range(15):
        flat = flat + rz[i]
    for g, owner in enumerate(owners):

        @pl.when(owner != z)
        def _(g=g, owner=owner):
            pltpu.make_async_remote_copy(
                src_ref=nf.at[g], dst_ref=nf.at[g], send_sem=ng_s.at[0], recv_sem=ng_r.at[g],
                device_id=(owner * 4 + y, ccd), device_id_type=MESH,
            ).wait_recv()

    def wide(pieces):
        return jnp.concatenate([jnp.broadcast_to(piece, (8, 128)) for piece in pieces], 1)

    edges = [nf[6], pltpu.roll(nf[6], 112, 1), pltpu.roll(nf[6], 96, 1)]

    def band(o, pair):
        g, s = (o, pair) if o < 3 else (pair // 2, 6 + pair % 2)
        return wide([nf[g, s : s + 1], nf[3 + g, s : s + 1], edges[g][s : s + 1]])

    bands = [{} for _ in range(4)]
    for o in range(4):
        for p, (a, b) in enumerate(PAIRS):
            bands[o][a, b] = bands[o][b, a] = band(o, p)
    inside = lax.broadcasted_iota(jnp.int32, (8, 384), 1) < jnp.minimum(KNOTS + HALO - 256 * pid, 256 + 2 * HALO)
    shifted = [flat, pltpu.roll(flat, 112, 1), pltpu.roll(flat, 96, 1)]
    rhs = [wide([flat[i : i + 1], flat[4 + i : 5 + i], shifted[i][3:4]]) for i in range(3)]
    scale = [RELAX / (ATT_RIDGE + bands[0][i, i]) for i in range(3)]
    coef = [jnp.where(inside, rhs[i] * scale[i], 0.0) for i in range(3)]
    for _ in range(1, SWEEPS):
        ahead = [[pltpu.roll(coef[i], 384 - o, 1) for i in range(3)] for o in range(1, 4)]
        fresh = []
        for i in range(3):
            product = coef[i] * ATT_RIDGE
            for k in range(3):
                product = product + bands[0][i, k] * coef[k]
            for o in range(1, 4):
                back = bands[o][i, 0] * coef[0] + bands[o][i, 1] * coef[1] + bands[o][i, 2] * coef[2]
                product = product + pltpu.roll(back, o, 1)
                for k in range(3):
                    product = product + bands[o][i, k] * ahead[o - 1][k]
            fresh.append(jnp.where(inside, coef[i] + scale[i] * (rhs[i] - product), 0.0))
        coef = fresh
    cp[:, 3:4, :] = jnp.zeros((2, 1, 128), F32)
    for i in range(3):
        moved = pltpu.roll(coef[i], 384 - HALO, 1)
        for t in range(2):
            cp[t, i : i + 1] = moved[0:1, t * 128 : (t + 1) * 128]
    for i, k in enumerate(steps32):
        send(cp, cb.at[pl.ds(2 * pid, 2)], cg_s.at[i], cg_r.at[i], plane(*k))
    for t in range(2):
        cb[2 * pid + t] = cp[t]
    cb[BLOCKS] = jnp.zeros((4, 128), F32)
    for i, (ky, kx, kc) in enumerate(steps32):
        sy, sx, sc = (y + 4 - ky) % 4, (x + 4 - kx) % 4, (core + 2 - kc) % 2
        slot = cb.at[pl.ds(2 * (sc * 16 + sy * 4 + sx), 2)]
        pltpu.make_async_remote_copy(
            src_ref=cp, dst_ref=slot, send_sem=cg_s.at[i], recv_sem=cg_r.at[i],
            device_id=(z * 4 + sy, sx * 2 + sc), device_id_type=MESH,
        ).wait_recv()
    att_o[...] = cb[src][0:3]
    att_out = pltpu.make_async_copy(att_o, att_h, out_sem.at[1])
    att_out.start()

    def final_step(t, carry):
        for pair in range(UNROLL // 2):
            p = t * (UNROLL // 2) + pair
            halves = []
            for b in range(2):
                d = 2 * p + b
                now = jnp.concatenate([cb[d], cb[d + 1]], 0)
                turned = [now] + [pltpu.roll(now, 128 - j, 1) for j in range(1, 4)]
                flip = [pltpu.roll(v, 4, 0) for v in turned]
                pair01 = jnp.where(
                    upper, now, jnp.where(lane < 127, flip[1], turned[1])
                )
                pair23 = jnp.where(
                    upper,
                    jnp.where(lane < 126, turned[2], flip[2]),
                    jnp.where(lane < 125, flip[3], turned[3]),
                )
                stacked = jnp.concatenate([pair01, pair23], 0)
                halves.append(jnp.concatenate(parts(stacked, 3), 0).astype(BF16))
            both = jnp.concatenate(halves, 1)
            picked = lax.dot_general(both, otk[p], NN, preferred_element_type=F32)
            picked = picked[0:16] + picked[16:32] + picked[32:48]
            for b in range(2):
                d = 2 * p + b
                own = picked[:, b * 128 : b * 128 + 128]
                b01 = jnp.where(upper, bb[0, pl.ds(d, 1), :], bb[1, pl.ds(d, 1), :])
                b23 = jnp.where(upper, bb[2, pl.ds(d, 1), :], bb[3, pl.ds(d, 1), :])
                terms = ax8[:, cols(d)] * (own[0:8] * b01 + own[8:16] * b23)
                predicted = jnp.sum(terms, 0, keepdims=True)
                res_o[pl.ds(d, 1), :] = jnp.where(
                    lane1 < cnt[0, d], resid[pl.ds(d, 1), :] - predicted, 0.0
                )
        return carry

    lax.fori_loop(0, BLOCKS // UNROLL, final_step, 0)
    res_out = pltpu.make_async_copy(res_o, res_h, out_sem.at[2])
    res_out.start()

    for copy in started:
        copy.wait_send()
    for g, owner in enumerate(owners):

        @pl.when(owner != z)
        def _(g=g, owner=owner):
            pltpu.make_async_remote_copy(
                src_ref=npc.at[g], dst_ref=nz.at[0], send_sem=nz_s.at[g], recv_sem=nz_r.at[0],
                device_id=(owner * 4 + y, ccd), device_id_type=MESH,
            ).wait_send()

    @pl.when(is_owner)
    def _():
        for k in zsteps:
            pltpu.make_async_remote_copy(
                src_ref=nf.at[mine], dst_ref=nf.at[mine], send_sem=ng_s.at[k - 1], recv_sem=ng_r.at[mine],
                device_id=along(k), device_id_type=MESH,
            ).wait_send()

    for copy in (params_out, att_out, res_out):
        copy.wait()


def write_out(params_i, att_i, res_i, params_o, att_o, res_o, params, attitude, residual, sems):
    held = (params, attitude, residual)
    inward = [pltpu.make_async_copy(a, b, sems.at[i]) for i, (a, b) in enumerate(zip((params_i, att_i, res_i), held))]
    outward = [pltpu.make_async_copy(a, b, sems.at[i + 3]) for i, (a, b) in enumerate(zip(held, (params_o, att_o, res_o)))]
    for copy in inward:
        copy.start()
    for there, back in zip(inward, outward):
        there.wait()
        back.start()
    for copy in outward:
        copy.wait()


def on_device(design, observed, weight, phase_frac, axis_factors, source_index, knot_index, counts):
    dma = pltpu.SemaphoreType.DMA
    vm = lambda *shape: pltpu.VMEM(shape, F32)
    square = lambda v: v.reshape(64, 128)
    params, attitude, residual = pl.pallas_call(
        kernel,
        out_shape=(
            jax.ShapeDtypeStruct((5, 1024), F32),
            jax.ShapeDtypeStruct((3, 128), F32),
            jax.ShapeDtypeStruct((64, 128), F32),
        ),
        in_specs=[pl.BlockSpec(memory_space=pl.ANY)] * 8,
        out_specs=(pl.BlockSpec(memory_space=pl.ANY),) * 3,
        scratch_shapes=[
            vm(5, 1024), vm(3, 128), vm(64, 128), dma((3,)),
            vm(5, 8192), vm(64, 128), vm(64, 128), vm(64, 128), vm(3, 8192),
            pltpu.VMEM((64, 128), jnp.int32), pltpu.VMEM((64, 128), jnp.int32), pltpu.SMEM((1, 64), jnp.int32), dma((8,)),
            pltpu.VMEM((256, 8192), BF16),
            pltpu.VMEM((32, 256, 256), BF16),
            vm(14, 64, 128), vm(64, 128), vm(8, 8192),
            pltpu.VMEM((UNROLL // 8, 256, 1024), BF16),
            vm(256, 256), vm(8, 24, 128), vm(7, 24, 128), vm(8, 8, 128),
            vm(TILES, 24, 128), vm(HALF, 24, 128), vm(16, 7, 8, 128), vm(15, 7, 8, 128),
            vm(7, 8, 128), vm(15, 8, 128), vm(7, 8, 128),
            vm(TILES, 4, 128), vm(HALF, 4, 128), vm(16, 3, 4, 128), vm(15, 3, 4, 128),
            vm(8, 128), vm(15, 8, 128), vm(2, 4, 128), vm(TILES, 4, 128), vm(64, 128),
            dma((7,)), dma((7,)), dma((7,)), dma((7,)),
            dma, dma, dma((15,)), dma((15,)), dma((7,)), dma((15,)), dma((15,)), dma((7,)),
            dma, dma, dma((15,)), dma((15,)), dma((15,)), dma((15,)), dma((31,)), dma((31,)),
        ],
        compiler_params=pltpu.CompilerParams(
            collective_id=0, has_side_effects=True, vmem_limit_bytes=60 * 1024 * 1024
        ),
    )(
        design, square(observed), square(weight), square(phase_frac), axis_factors,
        square(source_index), square(knot_index), counts.reshape(1, 64),
    )
    anywhere = pl.BlockSpec(memory_space=pl.ANY)
    params, attitude, residual = pl.pallas_call(
        write_out,
        out_shape=(
            jax.ShapeDtypeStruct((5, 1024), F32),
            jax.ShapeDtypeStruct((3, 128), F32),
            jax.ShapeDtypeStruct((64, 128), F32),
        ),
        in_specs=[anywhere] * 3,
        out_specs=(anywhere,) * 3,
        scratch_shapes=[vm(5, 1024), vm(3, 128), vm(64, 128), dma((6,))],
        compiler_params=pltpu.CompilerParams(vmem_limit_bytes=60 * 1024 * 1024),
    )(params, attitude, residual)
    return params, attitude, residual.reshape(8192)


def solution(mesh):
    rows = P(("src", "ccd"))
    wide = P(None, ("src", "ccd"))
    in_specs = (wide, rows, rows, rows, wide, rows, rows, P("src", "ccd", None))
    out_specs = (P(None, "src"), P(None, "src"), rows)
    return jax.shard_map(on_device, mesh=mesh, in_specs=in_specs, out_specs=out_specs, check_vma=False)
```

```python
import functools

import jax
import jax.numpy as jnp
from jax import lax
from jax.experimental import pallas as pl
from jax.experimental.pallas import tpu as pltpu
from jax.sharding import PartitionSpec as P

F32 = jnp.float32
BF16 = jnp.bfloat16
MESH = pl.DeviceIdType.MESH
SRC_RIDGE = 1.0
ATT_RIDGE = 1.0
RELAX = 0.15
SWEEPS = 3
BLOCKS = 64
TILES = 65
HALF = 33
KNOTS = 8192
HALO = 6
UNROLL = 16
LONG = 32
PAIRS = [(0, 0), (0, 1), (0, 2), (1, 1), (1, 2), (2, 2)]
NT = (((1,), (1,)), ((), ()))
NN = (((1,), (0,)), ((), ()))


def moment_row(m, n):
    m, n = min(m, n), max(m, n)
    return {0: n, 4: n + 2, 1: 7 + n, 3: 10 + n, 2: 14 + n}[m]


def parts(value, count):
    out = []
    rest = value
    for _ in range(count - 1):
        top = rest.astype(BF16).astype(F32)
        out.append(top)
        rest = rest - top
    out.append(rest)
    return out


def solve_rows(row):
    factor = {}
    inverse = {}
    for j in range(5):
        for i in range(j, 5):
            running = row(moment_row(j, i)) + (SRC_RIDGE if i == j else 0.0)
            for k in range(j):
                running = running - factor[i, k] * factor[j, k]
            if i == j:
                inverse[j] = 1.0 / jnp.sqrt(running)
            else:
                factor[i, j] = running * inverse[j]
    forward = []
    for i in range(5):
        running = row(moment_row(i, 5))
        for k in range(i):
            running = running - factor[i, k] * forward[k]
        forward.append(running * inverse[i])
    solved = [None] * 5
    for i in reversed(range(5)):
        running = forward[i]
        for k in range(i + 1, 5):
            running = running - factor[k, i] * solved[k]
        solved[i] = running * inverse[i]
    return solved


def kernel(
    design_h, obs_h, wt_h, ph_h, ax_h, sidx_h, kidx_h, cnt_h,
    params_h, att_h, res_h,
    params_o, att_o, res_o, out_sem,
    design, obs, wt, ph, ax, sidx, kidx, cnt, in_sem,
    otlo, otk, bb, wl, ax8, acc, mom, momr, par,
    nloc, nhalf, nsum, nr, npc, nz, nf,
    rloc, rhalf, rsum, rr, rpc, rz, cp, cb, resid,
    ma_s, ma_r, pa_s, pa_r, nh_s, nh_r, np_s, np_r, nz_s, nz_r, ng_s, ng_r,
    rh_s, rh_r, rp_s, rp_r, rz_s, rz_r, cg_s, cg_r,
):
    src = lax.axis_index("src")
    ccd = lax.axis_index("ccd")
    z, y = src // 4, src % 4
    x, core = ccd // 2, ccd % 2
    chip = y * 4 + x
    pid = core * 16 + chip

    def plane(ky, kx, kc):
        return z * 4 + (y + ky) % 4, ((x + kx) % 4) * 2 + (core + kc) % 2

    def along(kz):
        return ((z + kz) % 16) * 4 + y, ccd

    steps16 = [(2, 2), (2, 1), (2, 3), (1, 2), (3, 2), (2, 0), (0, 2), (1, 1), (3, 3), (1, 3), (3, 1), (1, 0), (3, 0), (0, 1), (0, 3)]
    steps32 = [(ky, kx, kc) for ky, kx in steps16 for kc in (1, 0)] + [(0, 0, 1)]
    zsteps = [8, 7, 9, 6, 10, 5, 11, 4, 12, 3, 13, 2, 14, 1, 15]

    loads = []
    held = (sidx, wt, design, obs, ph, ax, kidx)
    for i, (a, b) in enumerate(zip((sidx_h, wt_h, design_h, obs_h, ph_h, ax_h, kidx_h), held)):
        loads.append(pltpu.make_async_copy(a, b, in_sem.at[i]))
        loads[-1].start()

    loads.insert(0, pltpu.make_async_copy(cnt_h, cnt, in_sem.at[7]))
    loads[0].start()

    def send(a, b, ssem, rsem, to):
        copy = pltpu.make_async_remote_copy(
            src_ref=a, dst_ref=b, send_sem=ssem, recv_sem=rsem, device_id=to, device_id_type=MESH
        )
        copy.start()

    def settle(ref, sem):
        pltpu.make_async_copy(ref, ref, sem).wait()

    barrier = pltpu.get_barrier_semaphore()
    for k in steps32:
        pl.semaphore_signal(barrier, inc=1, device_id=plane(*k), device_id_type=MESH)
    for k in zsteps:
        pl.semaphore_signal(barrier, inc=1, device_id=along(k), device_id_type=MESH)

    lane = lax.broadcasted_iota(jnp.int32, (8, 128), 1)
    lane1 = lax.broadcasted_iota(jnp.int32, (1, 128), 1)
    sub = lax.broadcasted_iota(jnp.int32, (8, 128), 0)
    iota256 = lax.broadcasted_iota(jnp.int32, (256, 128), 0).astype(F32).astype(BF16)
    one, zero = jnp.ones((256, 128), BF16), jnp.zeros((256, 128), BF16)

    def cols(d):
        return pl.ds(pl.multiple_of(d * 128, 128), 128)

    def tall(row, count):
        packed = jnp.broadcast_to(row.astype(F32), (16, 128)).astype(BF16)
        return jnp.concatenate([packed] * count, 0)

    def hot(row, size):
        return jnp.where(iota256[:size] == tall(row, size // 16), one[:size], zero[:size])

    def dot(a, b, dims):
        return lax.dot_general(a, b, dims, precision=lax.Precision.DEFAULT, preferred_element_type=F32)

    for copy in loads[:5]:
        copy.wait()
    acc[...] = jnp.zeros_like(acc)

    def moments_step(t, carry):
        total = None
        for part in range(UNROLL // 8):
            lefts, hots = [], []
            for b in range(8):
                d = t * UNROLL + part * 8 + b
                s_row = sidx[pl.ds(d, 1), :]
                hots.append(hot(s_row & 255, 256))
                otlo[:, cols(d)] = hots[-1]
                high = tall(s_row >> 8, 4)
                w = jnp.where(lane1 < cnt[0, d], wt[pl.ds(d, 1), :], 0.0)
                wl[pl.ds(d, 1), :] = w
                e = jnp.concatenate([design[:, cols(d)], jnp.zeros((3, 128), F32)], 0)
                o = jnp.broadcast_to(obs[pl.ds(d, 1), :], (8, 128))
                e0, e1, e2, e3, e4 = [design[i : i + 1, cols(d)] for i in range(5)]
                down = pltpu.roll(e, 2, 0)
                ea = jnp.where(sub < 5, e, jnp.where(sub == 6, e4, o))
                eb = jnp.where(sub < 4, pltpu.roll(e, 7, 0), jnp.where((sub == 5) | (sub == 6), down, o))
                ec = jnp.where(sub < 3, pltpu.roll(e, 6, 0), jnp.where((sub > 3) & (sub < 7), down, o))
                ga = parts(w * ea * jnp.where(sub < 6, e0, e4), 3)
                gb = parts(w * eb * jnp.where(sub < 5, e1, e3), 3)
                gc = parts(w * ec * e2, 3)
                rows = [ga[0], gb[0], ga[1], gb[1], ga[2], gb[2], jnp.where(sub < 4, gc[0], gc[1]), gc[2]]
                stacked = jnp.concatenate(rows, 0).astype(BF16)
                masked = [jnp.where(high == jnp.full((64, 128), h, BF16), stacked, zero[:64]) for h in range(4)]
                lefts.append(jnp.concatenate(masked, 0))
            product = dot(jnp.concatenate(lefts, 1), jnp.concatenate(hots, 1), NT)
            total = product if total is None else total + product
        acc[...] += total
        return carry

    lax.fori_loop(0, BLOCKS // UNROLL, moments_step, 0)
    for h in range(4):
        v = [acc[64 * h + 8 * i : 64 * h + 8 * i + 8] for i in range(8)]
        tail = v[6] + pltpu.roll(v[6], 4, 0) + v[7]
        total = jnp.concatenate([v[0] + v[2] + v[4], v[1] + v[3] + v[5], tail], 0)
        mom[2 * h] = total[:, :128]
        mom[2 * h + 1] = total[:, 128:]
    pl.semaphore_wait(barrier, len(steps32) + len(zsteps))
    for k in (4, 5, 3, 2, 6, 7, 1):
        to = (ccd + k) % 8
        send(mom.at[to], momr.at[k - 1], ma_s, ma_r, (src, to))

    for copy in loads[5:]:
        copy.wait()
    u = ph[...]
    rem = 1.0 - u
    sq = u * u
    cu = sq * u
    basis = [
        rem * rem * rem / 6.0,
        (3.0 * cu - 6.0 * sq + 4.0) / 6.0,
        (-3.0 * cu + 3.0 * sq + 3.0 * u + 1.0) / 6.0,
        cu / 6.0,
    ]
    bbid = {}
    for i in range(4):
        bb[i] = basis[i]
    for i in range(4):
        for j in range(i, 4):
            bbid[i, j] = 4 + len(bbid)
            bb[bbid[i, j]] = basis[i] * basis[j]
    ax8[0:3, :] = ax[...]
    ax8[3:4, :] = jnp.zeros((1, KNOTS), F32)
    ax8[4:7, :] = ax[...]
    ax8[7:8, :] = jnp.zeros((1, KNOTS), F32)

    def spread_shift(value, shift):
        lanes = lax.broadcasted_iota(jnp.int32, value.shape, 1)
        turned = pltpu.roll(value, shift, 1)
        return jnp.where(lanes >= shift, turned, 0.0), jnp.where(lanes < shift, turned, 0.0)

    def normal_step(t, carry):
        for pair in range(UNROLL // 2):
            p = t * (UNROLL // 2) + pair
            halves, hots = [], []
            for b in range(2):
                d = 2 * p + b
                own = hot(kidx[pl.ds(d, 1), :], 128)
                hots.append(jnp.concatenate([own, zero[:128]] if b == 0 else [zero[:128], own], 0))
                w = wl[pl.ds(d, 1), :]
                a = [jnp.broadcast_to(ax[i : i + 1, cols(d)], (8, 128)) for i in range(3)]
                wa = [w * a[i] for i in range(3)]
                left = jnp.where(sub < 3, wa[0], jnp.where(sub < 5, wa[1], wa[2]))
                right = jnp.where(sub == 0, a[0], jnp.where((sub == 1) | (sub == 3), a[1], a[2]))
                only = jnp.where(sub < 6, left * right, 0.0)
                tails = [
                    wa[0] * jnp.where(sub == 6, a[0], a[1]),
                    jnp.where(sub == 6, wa[0], wa[1]) * jnp.where(sub == 6, a[2], a[1]),
                    a[2] * jnp.where(sub == 6, wa[1], wa[2]),
                ]

                def term(i, j):
                    return bb[bbid[i, j], pl.ds(d, 1), :]

                last = term(0, 3)
                groups = [jnp.where(sub < 6, only * term(0, o), tails[o] * last) for o in range(3)]
                groups += [only * term(1, 1), only * term(1, 2), only * term(1, 3)]
                groups += [only * term(2, 2), only * term(2, 3), only * term(3, 3)]
                stacked = jnp.concatenate(groups, 0)
                halves.append(jnp.concatenate(parts(stacked, 2), 0).astype(BF16))
            both = jnp.concatenate(halves, 1)
            hot2 = jnp.concatenate(hots, 1)
            otk[p] = hot2
            sums = dot(both, hot2, NT)
            sums = sums[:72] + sums[72:]
            zeros8 = jnp.zeros((8, 128), F32)
            zeros16 = jnp.zeros((16, 128), F32)
            for b in range(2):
                own = sums[:, b * 128 : b * 128 + 128]
                c0, v0 = spread_shift(own[0:24], HALO)
                c1, v1 = spread_shift(own[24:48], HALO + 1)
                c2, v2 = spread_shift(own[48:64], HALO + 2)
                c3, v3 = spread_shift(own[64:72], HALO + 3)
                here = c0 + c1 + jnp.concatenate([c2, zeros8], 0) + jnp.concatenate([c3, zeros16], 0)
                nloc[2 * p + b] = here + carry
                carry = v0 + v1 + jnp.concatenate([v2, zeros8], 0) + jnp.concatenate([v3, zeros16], 0)
        return carry

    nloc[BLOCKS] = lax.fori_loop(0, BLOCKS // UNROLL, normal_step, jnp.zeros((24, 128), F32))
    mate = (src, x * 2 + (core + 1) % 2)
    send(nloc.at[pl.ds(32 * ((core + 1) % 2), HALF)], nhalf, nh_s, nh_r, mate)

    settle(momr, ma_r)
    whole = mom[ccd]
    for k in range(7):
        whole = whole + momr[k]
    solved = solve_rows(lambda r: whole[r : r + 1])
    par[ccd] = jnp.concatenate(solved + [jnp.zeros((3, 128), F32)], 0)
    for k in (4, 5, 3, 2, 6, 7, 1):
        send(par.at[ccd], par.at[ccd], pa_s, pa_r, (src, (ccd + k) % 8))
    def pack(halo):
        near = jnp.where(lane < 32, pltpu.roll(halo[1], 16, 1), pltpu.roll(halo[2], 32, 1))
        return jnp.where(lane < 16, halo[0], near)

    settle(nhalf, nh_r)
    for i in range(16):
        for t in range(2):
            tile = nloc[32 * core + 2 * i + t] + nhalf[2 * i + t]
            for g in range(3):
                nsum[i, 3 * t + g] = tile[8 * g : 8 * g + 8]
        if i:
            nsum[i - 1, 6] = pack([nsum[i, g] for g in range(3)])
    tile = nloc[32 * core + 32] + nhalf[32]
    nsum[15, 6] = pack([tile[8 * g : 8 * g + 8] for g in range(3)])

    def to_owner(i):
        ky, kx = steps16[i]
        there = ((y + ky) % 4) * 4 + (x + kx) % 4
        send(nsum.at[there], nr.at[i], np_s, np_r, plane(ky, kx, 0))

    for i in range(15):
        to_owner(i)

    settle(par.at[0:7], pa_r)
    table = jnp.concatenate([jnp.concatenate([par[2 * h], par[2 * h + 1]], 1) for h in range(4)], 0)
    table = jnp.concatenate(parts(table, 3), 0).astype(BF16)
    upper = sub < 4

    def residual_step(t, carry):
        for part in range(LONG // 8):
            window = otlo[:, pl.ds(pl.multiple_of(t * LONG * 128 + part * 1024, 1024), 1024)]
            picked = dot(table, window, NN)
            picked = picked[0:32] + picked[32:64] + picked[64:96]
            for pair in range(4):
                halves = []
                p = t * (LONG // 2) + part * 4 + pair
                for b in range(2):
                    d = 2 * p + b
                    high = jnp.broadcast_to(sidx[pl.ds(d, 1), :] >> 8, (8, 128))
                    own = picked[:, pair * 256 + b * 128 : pair * 256 + b * 128 + 128]
                    chosen = own[0:8]
                    for h in range(1, 4):
                        chosen = jnp.where(high == h, own[8 * h : 8 * h + 8], chosen)
                    fitted = jnp.sum(chosen[0:5] * design[:, cols(d)], 0, keepdims=True)
                    r = jnp.where(lane1 < cnt[0, d], obs[pl.ds(d, 1), :] - fitted, 0.0)
                    resid[pl.ds(d, 1), :] = r
                    wr = jnp.broadcast_to(wl[pl.ds(d, 1), :] * r, (8, 128))
                    a = ax8[:, cols(d)] * wr
                    pair01 = a * jnp.where(upper, bb[0, pl.ds(d, 1), :], bb[1, pl.ds(d, 1), :])
                    pair23 = a * jnp.where(upper, bb[2, pl.ds(d, 1), :], bb[3, pl.ds(d, 1), :])
                    stacked = jnp.concatenate([pair01, pair23], 0)
                    halves.append(jnp.concatenate(parts(stacked, 3), 0).astype(BF16))
                both = jnp.concatenate(halves, 1)
                sums = dot(both, otk[p], NT)
                sums = sums[0:16] + sums[16:32] + sums[32:48]
                for b in range(2):
                    here = carry
                    over = jnp.zeros((8, 128), F32)
                    for g in range(2):
                        value = sums[8 * g : 8 * g + 8, b * 128 : b * 128 + 128]
                        first, second = HALO + 2 * g, HALO + 2 * g + 1
                        turned = jnp.where(upper, pltpu.roll(value, first, 1), pltpu.roll(value, second, 1))
                        limit = jnp.where(upper, first, second)
                        here = here + jnp.where(lane >= limit, turned, 0.0)
                        over = over + jnp.where(lane < limit, turned, 0.0)
                    folded = here + pltpu.roll(here, 4, 0)
                    rloc[2 * p + b] = folded[0:4]
                    carry = over
        return carry

    last = lax.fori_loop(0, BLOCKS // LONG, residual_step, jnp.zeros((8, 128), F32))
    last = last + pltpu.roll(last, 4, 0)
    rloc[BLOCKS] = last[0:4]

    send(rloc.at[pl.ds(32 * ((core + 1) % 2), HALF)], rhalf, rh_s, rh_r, mate)
    for c in range(8):
        params_o[:, c * 128 : (c + 1) * 128] = par[c, 0:5]
    params_out = pltpu.make_async_copy(params_o, params_h, out_sem.at[0])
    params_out.start()
    settle(rhalf, rh_r)
    for i in range(16):
        for t in range(2):
            rsum[i, t] = rloc[32 * core + 2 * i + t] + rhalf[2 * i + t]
        rsum[i, 2] = rloc[32 * core + 2 * i + 2] + rhalf[2 * i + 2]
    for i, (ky, kx) in enumerate(steps16):
        there = ((y + ky) % 4) * 4 + (x + kx) % 4
        send(rsum.at[there], rr.at[i], rp_s, rp_r, plane(ky, kx, 0))

    settle(nr, np_r)
    for g in range(7):
        total = nsum[chip, g]
        for i in range(15):
            total = total + nr[i, g]
        npc[g] = total
    owners = [(16 * g) // 7 for g in range(7)]
    mine = (7 * z + 15) // 16
    is_owner = (16 * mine) // 7 == z
    for g, owner in enumerate(owners):
        step = (owner + 16 - z) % 16

        @pl.when(owner != z)
        def _(g=g, owner=owner, step=step):
            pltpu.make_async_remote_copy(
                src_ref=npc.at[g], dst_ref=nz.at[step - 1], send_sem=nz_s, recv_sem=nz_r,
                device_id=(owner * 4 + y, ccd), device_id_type=MESH,
            ).start()

    settle(rr, rp_r)
    rows = []
    for t in range(3):
        total = rsum[chip, t]
        for i in range(15):
            total = total + rr[i, t]
        rows.append(total)
    low = jnp.concatenate(rows[:2], 0)
    edge = jnp.where(lane1 < 16, rows[2][0:1], jnp.where(lane1 < 32, pltpu.roll(rows[2], 16, 1)[1:2], pltpu.roll(rows[2], 32, 1)[2:3]))
    rpc[...] = jnp.where((sub == 3) | (sub == 7), jnp.broadcast_to(edge, (8, 128)), low)
    for kz in zsteps:
        send(rpc, rz.at[kz - 1], rz_s, rz_r, along(kz))

    @pl.when(is_owner)
    def _():
        total = npc[mine]
        settle(nz, nz_r)
        for k in range(15):
            total = total + nz[k]
        nf[mine] = total
        for k in zsteps:
            pltpu.make_async_remote_copy(
                src_ref=nf.at[mine], dst_ref=nf.at[mine], send_sem=ng_s, recv_sem=ng_r,
                device_id=along(k), device_id_type=MESH,
            ).start()

    settle(rz, rz_r)
    flat = rpc[...]
    for i in range(15):
        flat = flat + rz[i]
    @pl.when(is_owner)
    def _():
        settle(nf.at[0:6], ng_r)

    @pl.when(jnp.logical_not(is_owner))
    def _():
        settle(nf, ng_r)

    def wide(pieces):
        return jnp.concatenate([jnp.broadcast_to(piece, (8, 128)) for piece in pieces], 1)

    edges = [nf[6], pltpu.roll(nf[6], 112, 1), pltpu.roll(nf[6], 96, 1)]

    def band(o, pair):
        g, s = (o, pair) if o < 3 else (pair // 2, 6 + pair % 2)
        return wide([nf[g, s : s + 1], nf[3 + g, s : s + 1], edges[g][s : s + 1]])

    bands = [{} for _ in range(4)]
    for o in range(4):
        for p, (a, b) in enumerate(PAIRS):
            bands[o][a, b] = bands[o][b, a] = band(o, p)
    inside = lax.broadcasted_iota(jnp.int32, (8, 384), 1) < jnp.minimum(KNOTS + HALO - 256 * pid, 256 + 2 * HALO)
    shifted = [flat, pltpu.roll(flat, 112, 1), pltpu.roll(flat, 96, 1)]
    rhs = [wide([flat[i : i + 1], flat[4 + i : 5 + i], shifted[i][3:4]]) for i in range(3)]
    scale = [RELAX / (ATT_RIDGE + bands[0][i, i]) for i in range(3)]
    coef = [jnp.where(inside, rhs[i] * scale[i], 0.0) for i in range(3)]
    for _ in range(1, SWEEPS):
        ahead = [[pltpu.roll(coef[i], 384 - o, 1) for i in range(3)] for o in range(1, 4)]
        fresh = []
        for i in range(3):
            product = coef[i] * ATT_RIDGE
            for k in range(3):
                product = product + bands[0][i, k] * coef[k]
            for o in range(1, 4):
                back = bands[o][i, 0] * coef[0] + bands[o][i, 1] * coef[1] + bands[o][i, 2] * coef[2]
                product = product + pltpu.roll(back, o, 1)
                for k in range(3):
                    product = product + bands[o][i, k] * ahead[o - 1][k]
            fresh.append(jnp.where(inside, coef[i] + scale[i] * (rhs[i] - product), 0.0))
        coef = fresh
    cp[:, 3:4, :] = jnp.zeros((2, 1, 128), F32)
    for i in range(3):
        moved = pltpu.roll(coef[i], 384 - HALO, 1)
        for t in range(2):
            cp[t, i : i + 1] = moved[0:1, t * 128 : (t + 1) * 128]
    for i, k in enumerate(steps32):
        send(cp, cb.at[pl.ds(2 * pid, 2)], cg_s, cg_r, plane(*k))
    for t in range(2):
        cb[2 * pid + t] = cp[t]
    cb[BLOCKS] = jnp.zeros((4, 128), F32)
    settle(cb.at[0:62], cg_r)
    att_o[...] = cb[src][0:3]
    att_out = pltpu.make_async_copy(att_o, att_h, out_sem.at[1])
    att_out.start()

    def final_step(t, carry):
        for pair in range(LONG // 2):
            p = t * (LONG // 2) + pair
            halves = []
            for b in range(2):
                d = 2 * p + b
                now = jnp.concatenate([cb[d], cb[d + 1]], 0)
                turned = [now] + [pltpu.roll(now, 128 - j, 1) for j in range(1, 4)]
                flip = [pltpu.roll(v, 4, 0) for v in turned]
                pair01 = jnp.where(
                    upper, now, jnp.where(lane < 127, flip[1], turned[1])
                )
                pair23 = jnp.where(
                    upper,
                    jnp.where(lane < 126, turned[2], flip[2]),
                    jnp.where(lane < 125, flip[3], turned[3]),
                )
                stacked = jnp.concatenate([pair01, pair23], 0)
                halves.append(jnp.concatenate(parts(stacked, 3), 0).astype(BF16))
            both = jnp.concatenate(halves, 1)
            picked = dot(both, otk[p], NN)
            picked = picked[0:16] + picked[16:32] + picked[32:48]
            for b in range(2):
                d = 2 * p + b
                own = picked[:, b * 128 : b * 128 + 128]
                b01 = jnp.where(upper, bb[0, pl.ds(d, 1), :], bb[1, pl.ds(d, 1), :])
                b23 = jnp.where(upper, bb[2, pl.ds(d, 1), :], bb[3, pl.ds(d, 1), :])
                terms = ax8[:, cols(d)] * (own[0:8] * b01 + own[8:16] * b23)
                predicted = jnp.sum(terms, 0, keepdims=True)
                res_o[pl.ds(d, 1), :] = jnp.where(
                    lane1 < cnt[0, d], resid[pl.ds(d, 1), :] - predicted, 0.0
                )
        return carry

    lax.fori_loop(0, BLOCKS // LONG, final_step, 0)
    res_out = pltpu.make_async_copy(res_o, res_h, out_sem.at[2])
    res_out.start()

    settle(momr, ma_s)
    settle(par.at[0:7], pa_s)
    settle(nhalf, nh_s)
    settle(nr, np_s)
    settle(rhalf, rh_s)
    settle(rr, rp_s)
    settle(rz, rz_s)
    settle(cb.at[0:62], cg_s)

    @pl.when(is_owner)
    def _():
        settle(nz.at[0:6], nz_s)
        settle(nz, ng_s)

    @pl.when(jnp.logical_not(is_owner))
    def _():
        settle(nz.at[0:7], nz_s)

    for copy in (params_out, att_out, res_out):
        copy.wait()


def write_out(params_i, att_i, res_i, params_o, att_o, res_o, params, attitude, residual, sems):
    held = (params, attitude, residual)
    inward = [pltpu.make_async_copy(a, b, sems.at[i]) for i, (a, b) in enumerate(zip((params_i, att_i, res_i), held))]
    outward = [pltpu.make_async_copy(a, b, sems.at[i + 3]) for i, (a, b) in enumerate(zip(held, (params_o, att_o, res_o)))]
    for copy in inward:
        copy.start()
    for there, back in zip(inward, outward):
        there.wait()
        back.start()
    for copy in outward:
        copy.wait()


def on_device(design, observed, weight, phase_frac, axis_factors, source_index, knot_index, counts):
    dma = pltpu.SemaphoreType.DMA
    vm = lambda *shape: pltpu.VMEM(shape, F32)
    square = lambda v: v.reshape(64, 128)
    params, attitude, residual = pl.pallas_call(
        kernel,
        out_shape=(
            jax.ShapeDtypeStruct((5, 1024), F32),
            jax.ShapeDtypeStruct((3, 128), F32),
            jax.ShapeDtypeStruct((64, 128), F32),
        ),
        in_specs=[pl.BlockSpec(memory_space=pl.ANY)] * 8,
        out_specs=(pl.BlockSpec(memory_space=pl.ANY),) * 3,
        scratch_shapes=[
            vm(5, 1024), vm(3, 128), vm(64, 128), dma((3,)),
            vm(5, 8192), vm(64, 128), vm(64, 128), vm(64, 128), vm(3, 8192),
            pltpu.VMEM((64, 128), jnp.int32), pltpu.VMEM((64, 128), jnp.int32), pltpu.SMEM((1, 64), jnp.int32), dma((8,)),
            pltpu.VMEM((256, 8192), BF16),
            pltpu.VMEM((32, 256, 256), BF16),
            vm(14, 64, 128), vm(64, 128), vm(8, 8192),
            vm(256, 256), vm(8, 24, 128), vm(7, 24, 128), vm(8, 8, 128),
            vm(TILES, 24, 128), vm(HALF, 24, 128), vm(16, 7, 8, 128), vm(15, 7, 8, 128),
            vm(7, 8, 128), vm(15, 8, 128), vm(7, 8, 128),
            vm(TILES, 4, 128), vm(HALF, 4, 128), vm(16, 3, 4, 128), vm(15, 3, 4, 128),
            vm(8, 128), vm(15, 8, 128), vm(2, 4, 128), vm(TILES, 4, 128), vm(64, 128),
        ]
        + [dma] * 20,
        compiler_params=pltpu.CompilerParams(
            collective_id=0, has_side_effects=True, vmem_limit_bytes=60 * 1024 * 1024
        ),
    )(
        design, square(observed), square(weight), square(phase_frac), axis_factors,
        square(source_index), square(knot_index), counts.reshape(1, 64),
    )
    anywhere = pl.BlockSpec(memory_space=pl.ANY)
    params, attitude, residual = pl.pallas_call(
        write_out,
        out_shape=(
            jax.ShapeDtypeStruct((5, 1024), F32),
            jax.ShapeDtypeStruct((3, 128), F32),
            jax.ShapeDtypeStruct((64, 128), F32),
        ),
        in_specs=[anywhere] * 3,
        out_specs=(anywhere,) * 3,
        scratch_shapes=[vm(5, 1024), vm(3, 128), vm(64, 128), dma((6,))],
        compiler_params=pltpu.CompilerParams(vmem_limit_bytes=60 * 1024 * 1024),
    )(params, attitude, residual)
    return params, attitude, residual.reshape(8192)


def solution(mesh):
    rows = P(("src", "ccd"))
    wide = P(None, ("src", "ccd"))
    in_specs = (wide, rows, rows, rows, wide, rows, rows, P("src", "ccd", None))
    out_specs = (P(None, "src"), P(None, "src"), rows)
    return jax.shard_map(on_device, mesh=mesh, in_specs=in_specs, out_specs=out_specs, check_vma=False)
```

```python
import functools

import jax
import jax.numpy as jnp
from jax import lax
from jax.experimental import pallas as pl
from jax.experimental.pallas import tpu as pltpu
from jax.sharding import PartitionSpec as P

F32 = jnp.float32
BF16 = jnp.bfloat16
MESH = pl.DeviceIdType.MESH
SRC_RIDGE = 1.0
ATT_RIDGE = 1.0
RELAX = 0.15
SWEEPS = 3
BLOCKS = 64
TILES = 65
HALF = 33
KNOTS = 8192
HALO = 6
UNROLL = 16
LONG = 32
PAIRS = [(0, 0), (0, 1), (0, 2), (1, 1), (1, 2), (2, 2)]
NT = (((1,), (1,)), ((), ()))
NN = (((1,), (0,)), ((), ()))


def moment_row(m, n):
    m, n = min(m, n), max(m, n)
    return {0: n, 4: n + 2, 1: 7 + n, 3: 10 + n, 2: 14 + n}[m]


def parts(value, count):
    out = []
    rest = value
    for _ in range(count - 1):
        top = rest.astype(BF16).astype(F32)
        out.append(top)
        rest = rest - top
    out.append(rest)
    return out


def solve_rows(row):
    factor = {}
    inverse = {}
    for j in range(5):
        for i in range(j, 5):
            running = row(moment_row(j, i)) + (SRC_RIDGE if i == j else 0.0)
            for k in range(j):
                running = running - factor[i, k] * factor[j, k]
            if i == j:
                inverse[j] = 1.0 / jnp.sqrt(running)
            else:
                factor[i, j] = running * inverse[j]
    forward = []
    for i in range(5):
        running = row(moment_row(i, 5))
        for k in range(i):
            running = running - factor[i, k] * forward[k]
        forward.append(running * inverse[i])
    solved = [None] * 5
    for i in reversed(range(5)):
        running = forward[i]
        for k in range(i + 1, 5):
            running = running - factor[k, i] * solved[k]
        solved[i] = running * inverse[i]
    return solved


def kernel(
    design_h, obs_h, wt_h, ph_h, ax_h, sidx_h, kidx_h, cnt_h,
    params_h, att_h, res_h,
    params_o, att_o, res_o, out_sem,
    design, obs, wt, ph, ax, sidx, kidx, cnt, in_sem,
    otlo, otk, bb, wl, ax8, acc, mom, momr, par,
    nloc, nhalf, nsum, nr, npc, nz, nf,
    rloc, rhalf, rsum, rr, rpc, rz, cp, cb, resid,
    ma_s, ma_r, pa_s, pa_r, nh_s, nh_r, np_s, np_r, nz_s, nz_r, ng_s, ng_r,
    rh_s, rh_r, rp_s, rp_r, rz_s, rz_r, cg_s, cg_r, from_low, from_high,
):
    src = lax.axis_index("src")
    ccd = lax.axis_index("ccd")
    z, y = src // 4, src % 4
    x, core = ccd // 2, ccd % 2
    chip = y * 4 + x
    pid = core * 16 + chip

    def plane(ky, kx, kc):
        return z * 4 + (y + ky) % 4, ((x + kx) % 4) * 2 + (core + kc) % 2

    def along(kz):
        return ((z + kz) % 16) * 4 + y, ccd

    steps16 = [(2, 2), (2, 1), (2, 3), (1, 2), (3, 2), (2, 0), (0, 2), (1, 1), (3, 3), (1, 3), (3, 1), (1, 0), (3, 0), (0, 1), (0, 3)]
    steps32 = [(ky, kx, kc) for ky, kx in steps16 for kc in (1, 0)] + [(0, 0, 1)]
    zsteps = [8, 7, 9, 6, 10, 5, 11, 4, 12, 3, 13, 2, 14, 1, 15]

    loads = []
    held = (sidx, wt, design, obs, ph, ax, kidx)
    for i, (a, b) in enumerate(zip((sidx_h, wt_h, design_h, obs_h, ph_h, ax_h, kidx_h), held)):
        loads.append(pltpu.make_async_copy(a, b, in_sem.at[i]))
        loads[-1].start()

    loads.insert(0, pltpu.make_async_copy(cnt_h, cnt, in_sem.at[7]))
    loads[0].start()

    def send(a, b, ssem, rsem, to):
        copy = pltpu.make_async_remote_copy(
            src_ref=a, dst_ref=b, send_sem=ssem, recv_sem=rsem, device_id=to, device_id_type=MESH
        )
        copy.start()

    def settle(ref, sem):
        pltpu.make_async_copy(ref, ref, sem).wait()

    barrier = pltpu.get_barrier_semaphore()
    for k in steps32:
        pl.semaphore_signal(barrier, inc=1, device_id=plane(*k), device_id_type=MESH)
    for k in (1, 15):
        pl.semaphore_signal(barrier, inc=1, device_id=along(k), device_id_type=MESH)

    def tell():
        pl.semaphore_signal(from_low, inc=1, device_id=along(1), device_id_type=MESH)
        pl.semaphore_signal(from_high, inc=1, device_id=along(15), device_id_type=MESH)

    def heard(last=False):
        pl.semaphore_wait(from_low, 1)
        pl.semaphore_wait(from_high, 1)
        if not last:
            tell()


    lane = lax.broadcasted_iota(jnp.int32, (8, 128), 1)
    lane1 = lax.broadcasted_iota(jnp.int32, (1, 128), 1)
    sub = lax.broadcasted_iota(jnp.int32, (8, 128), 0)
    iota256 = lax.broadcasted_iota(jnp.int32, (256, 128), 0).astype(F32).astype(BF16)
    one, zero = jnp.ones((256, 128), BF16), jnp.zeros((256, 128), BF16)

    def cols(d):
        return pl.ds(pl.multiple_of(d * 128, 128), 128)

    def tall(row, count):
        packed = jnp.broadcast_to(row.astype(F32), (16, 128)).astype(BF16)
        return jnp.concatenate([packed] * count, 0)

    def hot(row, size):
        return jnp.where(iota256[:size] == tall(row, size // 16), one[:size], zero[:size])

    def dot(a, b, dims):
        return lax.dot_general(a, b, dims, precision=lax.Precision.DEFAULT, preferred_element_type=F32)

    for copy in loads[:5]:
        copy.wait()
    acc[...] = jnp.zeros_like(acc)

    def moments_step(t, carry):
        total = None
        for part in range(LONG // 8):
            lefts, hots = [], []
            for b in range(8):
                d = t * LONG + part * 8 + b
                s_row = sidx[pl.ds(d, 1), :]
                hots.append(hot(s_row & 255, 256))
                otlo[:, cols(d)] = hots[-1]
                high = tall(s_row >> 8, 4)
                w = jnp.where(lane1 < cnt[0, d], wt[pl.ds(d, 1), :], 0.0)
                wl[pl.ds(d, 1), :] = w
                e = jnp.concatenate([design[:, cols(d)], jnp.zeros((3, 128), F32)], 0)
                o = jnp.broadcast_to(obs[pl.ds(d, 1), :], (8, 128))
                e0, e1, e2, e3, e4 = [design[i : i + 1, cols(d)] for i in range(5)]
                down = pltpu.roll(e, 2, 0)
                ea = jnp.where(sub < 5, e, jnp.where(sub == 6, e4, o))
                eb = jnp.where(sub < 4, pltpu.roll(e, 7, 0), jnp.where((sub == 5) | (sub == 6), down, o))
                ec = jnp.where(sub < 3, pltpu.roll(e, 6, 0), jnp.where((sub > 3) & (sub < 7), down, o))
                ga = parts(w * ea * jnp.where(sub < 6, e0, e4), 3)
                gb = parts(w * eb * jnp.where(sub < 5, e1, e3), 3)
                gc = parts(w * ec * e2, 3)
                rows = [ga[0], gb[0], ga[1], gb[1], ga[2], gb[2], jnp.where(sub < 4, gc[0], gc[1]), gc[2]]
                stacked = jnp.concatenate(rows, 0).astype(BF16)
                masked = [jnp.where(high == jnp.full((64, 128), h, BF16), stacked, zero[:64]) for h in range(4)]
                lefts.append(jnp.concatenate(masked, 0))
            product = dot(jnp.concatenate(lefts, 1), jnp.concatenate(hots, 1), NT)
            total = product if total is None else total + product
        acc[...] += total
        return carry

    lax.fori_loop(0, BLOCKS // LONG, moments_step, 0)
    for h in range(4):
        v = [acc[64 * h + 8 * i : 64 * h + 8 * i + 8] for i in range(8)]
        tail = v[6] + pltpu.roll(v[6], 4, 0) + v[7]
        total = jnp.concatenate([v[0] + v[2] + v[4], v[1] + v[3] + v[5], tail], 0)
        mom[2 * h] = total[:, :128]
        mom[2 * h + 1] = total[:, 128:]
    pl.semaphore_wait(barrier, len(steps32) + 2)
    tell()
    for k in (4, 5, 3, 2, 6, 7, 1):
        to = (ccd + k) % 8
        send(mom.at[to], momr.at[k - 1], ma_s, ma_r, (src, to))

    for copy in loads[5:]:
        copy.wait()
    u = ph[...]
    rem = 1.0 - u
    sq = u * u
    cu = sq * u
    basis = [
        rem * rem * rem / 6.0,
        (3.0 * cu - 6.0 * sq + 4.0) / 6.0,
        (-3.0 * cu + 3.0 * sq + 3.0 * u + 1.0) / 6.0,
        cu / 6.0,
    ]
    bbid = {}
    for i in range(4):
        bb[i] = basis[i]
    for i in range(4):
        for j in range(i, 4):
            bbid[i, j] = 4 + len(bbid)
            bb[bbid[i, j]] = basis[i] * basis[j]
    ax8[0:3, :] = ax[...]
    ax8[3:4, :] = jnp.zeros((1, KNOTS), F32)
    ax8[4:7, :] = ax[...]
    ax8[7:8, :] = jnp.zeros((1, KNOTS), F32)

    def spread_shift(value, shift):
        lanes = lax.broadcasted_iota(jnp.int32, value.shape, 1)
        turned = pltpu.roll(value, shift, 1)
        return jnp.where(lanes >= shift, turned, 0.0), jnp.where(lanes < shift, turned, 0.0)

    def normal_step(t, carry):
        for pair in range(UNROLL // 2):
            p = t * (UNROLL // 2) + pair
            halves, hots = [], []
            for b in range(2):
                d = 2 * p + b
                own = hot(kidx[pl.ds(d, 1), :], 128)
                hots.append(jnp.concatenate([own, zero[:128]] if b == 0 else [zero[:128], own], 0))
                w = wl[pl.ds(d, 1), :]
                a = [jnp.broadcast_to(ax[i : i + 1, cols(d)], (8, 128)) for i in range(3)]
                wa = [w * a[i] for i in range(3)]
                left = jnp.where(sub < 3, wa[0], jnp.where(sub < 5, wa[1], wa[2]))
                right = jnp.where(sub == 0, a[0], jnp.where((sub == 1) | (sub == 3), a[1], a[2]))
                only = jnp.where(sub < 6, left * right, 0.0)
                tails = [
                    wa[0] * jnp.where(sub == 6, a[0], a[1]),
                    jnp.where(sub == 6, wa[0], wa[1]) * jnp.where(sub == 6, a[2], a[1]),
                    a[2] * jnp.where(sub == 6, wa[1], wa[2]),
                ]

                def term(i, j):
                    return bb[bbid[i, j], pl.ds(d, 1), :]

                last = term(0, 3)
                groups = [jnp.where(sub < 6, only * term(0, o), tails[o] * last) for o in range(3)]
                groups += [only * term(1, 1), only * term(1, 2), only * term(1, 3)]
                groups += [only * term(2, 2), only * term(2, 3), only * term(3, 3)]
                stacked = jnp.concatenate(groups, 0)
                halves.append(jnp.concatenate(parts(stacked, 2), 0).astype(BF16))
            both = jnp.concatenate(halves, 1)
            hot2 = jnp.concatenate(hots, 1)
            otk[p] = hot2
            sums = dot(both, hot2, NT)
            sums = sums[:72] + sums[72:]
            zeros8 = jnp.zeros((8, 128), F32)
            zeros16 = jnp.zeros((16, 128), F32)
            for b in range(2):
                own = sums[:, b * 128 : b * 128 + 128]
                c0, v0 = spread_shift(own[0:24], HALO)
                c1, v1 = spread_shift(own[24:48], HALO + 1)
                c2, v2 = spread_shift(own[48:64], HALO + 2)
                c3, v3 = spread_shift(own[64:72], HALO + 3)
                here = c0 + c1 + jnp.concatenate([c2, zeros8], 0) + jnp.concatenate([c3, zeros16], 0)
                nloc[2 * p + b] = here + carry
                carry = v0 + v1 + jnp.concatenate([v2, zeros8], 0) + jnp.concatenate([v3, zeros16], 0)
        return carry

    mate = (src, x * 2 + (core + 1) % 2)
    empty = jnp.zeros((24, 128), F32)
    nloc[BLOCKS] = empty
    carried = lax.fori_loop(0, 3, lambda t, c: normal_step(t + 1 - core, c), empty)
    nloc[64 - 16 * core] = carried
    send(nloc.at[pl.ds(32 * ((core + 1) % 2), HALF)], nhalf, nh_s, nh_r, mate)
    heard()
    carried = normal_step(3 * core, jnp.where(core == 1, carried, 0.0))
    nloc[16 + 48 * core] = nloc[16 + 48 * core] + carried

    heard()
    settle(momr, ma_r)
    whole = mom[ccd]
    for k in range(7):
        whole = whole + momr[k]
    solved = solve_rows(lambda r: whole[r : r + 1])
    par[ccd] = jnp.concatenate(solved + [jnp.zeros((3, 128), F32)], 0)
    for k in (4, 5, 3, 2, 6, 7, 1):
        send(par.at[ccd], par.at[ccd], pa_s, pa_r, (src, (ccd + k) % 8))
    def pack(halo):
        near = jnp.where(lane < 32, pltpu.roll(halo[1], 16, 1), pltpu.roll(halo[2], 32, 1))
        return jnp.where(lane < 16, halo[0], near)

    settle(nhalf, nh_r)
    for i in range(16):
        for t in range(2):
            tile = nloc[32 * core + 2 * i + t] + nhalf[2 * i + t]
            for g in range(3):
                nsum[i, 3 * t + g] = tile[8 * g : 8 * g + 8]
        if i:
            nsum[i - 1, 6] = pack([nsum[i, g] for g in range(3)])
    tile = nloc[32 * core + 32] + nhalf[32]
    nsum[15, 6] = pack([tile[8 * g : 8 * g + 8] for g in range(3)])

    def to_owner(i):
        ky, kx = steps16[i]
        there = ((y + ky) % 4) * 4 + (x + kx) % 4
        send(nsum.at[there], nr.at[i], np_s, np_r, plane(ky, kx, 0))

    for i in range(15):
        to_owner(i)
    heard()

    settle(par.at[0:7], pa_r)
    heard()
    table = jnp.concatenate([jnp.concatenate([par[2 * h], par[2 * h + 1]], 1) for h in range(4)], 0)
    table = jnp.concatenate(parts(table, 3), 0).astype(BF16)
    upper = sub < 4

    def residual_step(t, carry):
        for part in range(LONG // 8):
            window = otlo[:, pl.ds(pl.multiple_of(t * LONG * 128 + part * 1024, 1024), 1024)]
            picked = dot(table, window, NN)
            picked = picked[0:32] + picked[32:64] + picked[64:96]
            for pair in range(4):
                halves = []
                p = t * (LONG // 2) + part * 4 + pair
                for b in range(2):
                    d = 2 * p + b
                    high = jnp.broadcast_to(sidx[pl.ds(d, 1), :] >> 8, (8, 128))
                    own = picked[:, pair * 256 + b * 128 : pair * 256 + b * 128 + 128]
                    chosen = own[0:8]
                    for h in range(1, 4):
                        chosen = jnp.where(high == h, own[8 * h : 8 * h + 8], chosen)
                    fitted = jnp.sum(chosen[0:5] * design[:, cols(d)], 0, keepdims=True)
                    r = jnp.where(lane1 < cnt[0, d], obs[pl.ds(d, 1), :] - fitted, 0.0)
                    resid[pl.ds(d, 1), :] = r
                    wr = jnp.broadcast_to(wl[pl.ds(d, 1), :] * r, (8, 128))
                    a = ax8[:, cols(d)] * wr
                    pair01 = a * jnp.where(upper, bb[0, pl.ds(d, 1), :], bb[1, pl.ds(d, 1), :])
                    pair23 = a * jnp.where(upper, bb[2, pl.ds(d, 1), :], bb[3, pl.ds(d, 1), :])
                    stacked = jnp.concatenate([pair01, pair23], 0)
                    halves.append(jnp.concatenate(parts(stacked, 3), 0).astype(BF16))
                both = jnp.concatenate(halves, 1)
                sums = dot(both, otk[p], NT)
                sums = sums[0:16] + sums[16:32] + sums[32:48]
                for b in range(2):
                    here = carry
                    over = jnp.zeros((8, 128), F32)
                    for g in range(2):
                        value = sums[8 * g : 8 * g + 8, b * 128 : b * 128 + 128]
                        first, second = HALO + 2 * g, HALO + 2 * g + 1
                        turned = jnp.where(upper, pltpu.roll(value, first, 1), pltpu.roll(value, second, 1))
                        limit = jnp.where(upper, first, second)
                        here = here + jnp.where(lane >= limit, turned, 0.0)
                        over = over + jnp.where(lane < limit, turned, 0.0)
                    folded = here + pltpu.roll(here, 4, 0)
                    rloc[2 * p + b] = folded[0:4]
                    carry = over
        return carry

    last = lax.fori_loop(0, BLOCKS // LONG, residual_step, jnp.zeros((8, 128), F32))
    last = last + pltpu.roll(last, 4, 0)
    rloc[BLOCKS] = last[0:4]

    send(rloc.at[pl.ds(32 * ((core + 1) % 2), HALF)], rhalf, rh_s, rh_r, mate)
    heard()
    for c in range(8):
        params_o[:, c * 128 : (c + 1) * 128] = par[c, 0:5]
    params_out = pltpu.make_async_copy(params_o, params_h, out_sem.at[0])
    params_out.start()
    settle(rhalf, rh_r)
    for i in range(16):
        for t in range(2):
            rsum[i, t] = rloc[32 * core + 2 * i + t] + rhalf[2 * i + t]
        rsum[i, 2] = rloc[32 * core + 2 * i + 2] + rhalf[2 * i + 2]
    for i, (ky, kx) in enumerate(steps16):
        there = ((y + ky) % 4) * 4 + (x + kx) % 4
        send(rsum.at[there], rr.at[i], rp_s, rp_r, plane(ky, kx, 0))

    heard()
    settle(nr, np_r)
    for g in range(7):
        total = nsum[chip, g]
        for i in range(15):
            total = total + nr[i, g]
        npc[g] = total
    heard(last=True)
    owners = [(16 * g) // 7 for g in range(7)]
    mine = (7 * z + 15) // 16
    is_owner = (16 * mine) // 7 == z
    for g, owner in enumerate(owners):
        step = (owner + 16 - z) % 16

        @pl.when(owner != z)
        def _(g=g, owner=owner, step=step):
            pltpu.make_async_remote_copy(
                src_ref=npc.at[g], dst_ref=nz.at[step - 1], send_sem=nz_s, recv_sem=nz_r,
                device_id=(owner * 4 + y, ccd), device_id_type=MESH,
            ).start()

    settle(rr, rp_r)
    rows = []
    for t in range(3):
        total = rsum[chip, t]
        for i in range(15):
            total = total + rr[i, t]
        rows.append(total)
    low = jnp.concatenate(rows[:2], 0)
    edge = jnp.where(lane1 < 16, rows[2][0:1], jnp.where(lane1 < 32, pltpu.roll(rows[2], 16, 1)[1:2], pltpu.roll(rows[2], 32, 1)[2:3]))
    rpc[...] = jnp.where((sub == 3) | (sub == 7), jnp.broadcast_to(edge, (8, 128)), low)
    for kz in zsteps:
        send(rpc, rz.at[kz - 1], rz_s, rz_r, along(kz))

    @pl.when(is_owner)
    def _():
        total = npc[mine]
        settle(nz, nz_r)
        for k in range(15):
            total = total + nz[k]
        nf[mine] = total
        for k in zsteps:
            pltpu.make_async_remote_copy(
                src_ref=nf.at[mine], dst_ref=nf.at[mine], send_sem=ng_s, recv_sem=ng_r,
                device_id=along(k), device_id_type=MESH,
            ).start()

    settle(rz, rz_r)
    flat = rpc[...]
    for i in range(15):
        flat = flat + rz[i]
    @pl.when(is_owner)
    def _():
        settle(nf.at[0:6], ng_r)

    @pl.when(jnp.logical_not(is_owner))
    def _():
        settle(nf, ng_r)

    def wide(pieces):
        return jnp.concatenate([jnp.broadcast_to(piece, (8, 128)) for piece in pieces], 1)

    edges = [nf[6], pltpu.roll(nf[6], 112, 1), pltpu.roll(nf[6], 96, 1)]

    def band(o, pair):
        g, s = (o, pair) if o < 3 else (pair // 2, 6 + pair % 2)
        return wide([nf[g, s : s + 1], nf[3 + g, s : s + 1], edges[g][s : s + 1]])

    bands = [{} for _ in range(4)]
    for o in range(4):
        for p, (a, b) in enumerate(PAIRS):
            bands[o][a, b] = bands[o][b, a] = band(o, p)
    inside = lax.broadcasted_iota(jnp.int32, (8, 384), 1) < jnp.minimum(KNOTS + HALO - 256 * pid, 256 + 2 * HALO)
    shifted = [flat, pltpu.roll(flat, 112, 1), pltpu.roll(flat, 96, 1)]
    rhs = [wide([flat[i : i + 1], flat[4 + i : 5 + i], shifted[i][3:4]]) for i in range(3)]
    scale = [RELAX / (ATT_RIDGE + bands[0][i, i]) for i in range(3)]
    coef = [jnp.where(inside, rhs[i] * scale[i], 0.0) for i in range(3)]
    for _ in range(1, SWEEPS):
        ahead = [[pltpu.roll(coef[i], 384 - o, 1) for i in range(3)] for o in range(1, 4)]
        fresh = []
        for i in range(3):
            product = coef[i] * ATT_RIDGE
            for k in range(3):
                product = product + bands[0][i, k] * coef[k]
            for o in range(1, 4):
                back = bands[o][i, 0] * coef[0] + bands[o][i, 1] * coef[1] + bands[o][i, 2] * coef[2]
                product = product + pltpu.roll(back, o, 1)
                for k in range(3):
                    product = product + bands[o][i, k] * ahead[o - 1][k]
            fresh.append(jnp.where(inside, coef[i] + scale[i] * (rhs[i] - product), 0.0))
        coef = fresh
    cp[:, 3:4, :] = jnp.zeros((2, 1, 128), F32)
    for i in range(3):
        moved = pltpu.roll(coef[i], 384 - HALO, 1)
        for t in range(2):
            cp[t, i : i + 1] = moved[0:1, t * 128 : (t + 1) * 128]
    for i, k in enumerate(steps32):
        send(cp, cb.at[pl.ds(2 * pid, 2)], cg_s, cg_r, plane(*k))
    for t in range(2):
        cb[2 * pid + t] = cp[t]
    cb[BLOCKS] = jnp.zeros((4, 128), F32)
    settle(cb.at[0:62], cg_r)
    att_o[...] = cb[src][0:3]
    att_out = pltpu.make_async_copy(att_o, att_h, out_sem.at[1])
    att_out.start()

    def final_step(t, carry):
        for pair in range(LONG // 2):
            p = t * (LONG // 2) + pair
            halves = []
            for b in range(2):
                d = 2 * p + b
                now = jnp.concatenate([cb[d], cb[d + 1]], 0)
                turned = [now] + [pltpu.roll(now, 128 - j, 1) for j in range(1, 4)]
                flip = [pltpu.roll(v, 4, 0) for v in turned]
                pair01 = jnp.where(
                    upper, now, jnp.where(lane < 127, flip[1], turned[1])
                )
                pair23 = jnp.where(
                    upper,
                    jnp.where(lane < 126, turned[2], flip[2]),
                    jnp.where(lane < 125, flip[3], turned[3]),
                )
                stacked = jnp.concatenate([pair01, pair23], 0)
                halves.append(jnp.concatenate(parts(stacked, 3), 0).astype(BF16))
            both = jnp.concatenate(halves, 1)
            picked = dot(both, otk[p], NN)
            picked = picked[0:16] + picked[16:32] + picked[32:48]
            for b in range(2):
                d = 2 * p + b
                own = picked[:, b * 128 : b * 128 + 128]
                b01 = jnp.where(upper, bb[0, pl.ds(d, 1), :], bb[1, pl.ds(d, 1), :])
                b23 = jnp.where(upper, bb[2, pl.ds(d, 1), :], bb[3, pl.ds(d, 1), :])
                terms = ax8[:, cols(d)] * (own[0:8] * b01 + own[8:16] * b23)
                predicted = jnp.sum(terms, 0, keepdims=True)
                res_o[pl.ds(d, 1), :] = jnp.where(
                    lane1 < cnt[0, d], resid[pl.ds(d, 1), :] - predicted, 0.0
                )
        return carry

    lax.fori_loop(0, BLOCKS // LONG, final_step, 0)
    res_out = pltpu.make_async_copy(res_o, res_h, out_sem.at[2])
    res_out.start()

    settle(momr, ma_s)
    settle(par.at[0:7], pa_s)
    settle(nhalf, nh_s)
    settle(nr, np_s)
    settle(rhalf, rh_s)
    settle(rr, rp_s)
    settle(rz, rz_s)
    settle(cb.at[0:62], cg_s)

    @pl.when(is_owner)
    def _():
        settle(nz.at[0:6], nz_s)
        settle(nz, ng_s)

    @pl.when(jnp.logical_not(is_owner))
    def _():
        settle(nz.at[0:7], nz_s)

    for copy in (params_out, att_out, res_out):
        copy.wait()


def write_out(params_i, att_i, res_i, params_o, att_o, res_o, params, attitude, residual, sems):
    held = (params, attitude, residual)
    inward = [pltpu.make_async_copy(a, b, sems.at[i]) for i, (a, b) in enumerate(zip((params_i, att_i, res_i), held))]
    outward = [pltpu.make_async_copy(a, b, sems.at[i + 3]) for i, (a, b) in enumerate(zip(held, (params_o, att_o, res_o)))]
    for copy in inward:
        copy.start()
    for there, back in zip(inward, outward):
        there.wait()
        back.start()
    for copy in outward:
        copy.wait()


def on_device(design, observed, weight, phase_frac, axis_factors, source_index, knot_index, counts):
    dma = pltpu.SemaphoreType.DMA
    vm = lambda *shape: pltpu.VMEM(shape, F32)
    square = lambda v: v.reshape(64, 128)
    params, attitude, residual = pl.pallas_call(
        kernel,
        out_shape=(
            jax.ShapeDtypeStruct((5, 1024), F32),
            jax.ShapeDtypeStruct((3, 128), F32),
            jax.ShapeDtypeStruct((64, 128), F32),
        ),
        in_specs=[pl.BlockSpec(memory_space=pl.ANY)] * 8,
        out_specs=(pl.BlockSpec(memory_space=pl.ANY),) * 3,
        scratch_shapes=[
            vm(5, 1024), vm(3, 128), vm(64, 128), dma((3,)),
            vm(5, 8192), vm(64, 128), vm(64, 128), vm(64, 128), vm(3, 8192),
            pltpu.VMEM((64, 128), jnp.int32), pltpu.VMEM((64, 128), jnp.int32), pltpu.SMEM((1, 64), jnp.int32), dma((8,)),
            pltpu.VMEM((256, 8192), BF16),
            pltpu.VMEM((32, 256, 256), BF16),
            vm(14, 64, 128), vm(64, 128), vm(8, 8192),
            vm(256, 256), vm(8, 24, 128), vm(7, 24, 128), vm(8, 8, 128),
            vm(TILES, 24, 128), vm(HALF, 24, 128), vm(16, 7, 8, 128), vm(15, 7, 8, 128),
            vm(7, 8, 128), vm(15, 8, 128), vm(7, 8, 128),
            vm(TILES, 4, 128), vm(HALF, 4, 128), vm(16, 3, 4, 128), vm(15, 3, 4, 128),
            vm(8, 128), vm(15, 8, 128), vm(2, 4, 128), vm(TILES, 4, 128), vm(64, 128),
        ]
        + [dma] * 20
        + [pltpu.SemaphoreType.REGULAR] * 2,
        compiler_params=pltpu.CompilerParams(
            collective_id=0, has_side_effects=True, vmem_limit_bytes=60 * 1024 * 1024
        ),
    )(
        design, square(observed), square(weight), square(phase_frac), axis_factors,
        square(source_index), square(knot_index), counts.reshape(1, 64),
    )
    anywhere = pl.BlockSpec(memory_space=pl.ANY)
    params, attitude, residual = pl.pallas_call(
        write_out,
        out_shape=(
            jax.ShapeDtypeStruct((5, 1024), F32),
            jax.ShapeDtypeStruct((3, 128), F32),
            jax.ShapeDtypeStruct((64, 128), F32),
        ),
        in_specs=[anywhere] * 3,
        out_specs=(anywhere,) * 3,
        scratch_shapes=[vm(5, 1024), vm(3, 128), vm(64, 128), dma((6,))],
        compiler_params=pltpu.CompilerParams(vmem_limit_bytes=60 * 1024 * 1024),
    )(params, attitude, residual)
    return params, attitude, residual.reshape(8192)


def solution(mesh):
    rows = P(("src", "ccd"))
    wide = P(None, ("src", "ccd"))
    in_specs = (wide, rows, rows, rows, wide, rows, rows, P("src", "ccd", None))
    out_specs = (P(None, "src"), P(None, "src"), rows)
    return jax.shard_map(on_device, mesh=mesh, in_specs=in_specs, out_specs=out_specs, check_vma=False)
```

```python
import functools

import jax
import jax.numpy as jnp
from jax import lax
from jax.experimental import pallas as pl
from jax.experimental.pallas import tpu as pltpu
from jax.sharding import PartitionSpec as P

F32 = jnp.float32
BF16 = jnp.bfloat16
MESH = pl.DeviceIdType.MESH
SRC_RIDGE = 1.0
ATT_RIDGE = 1.0
RELAX = 0.15
SWEEPS = 3
BLOCKS = 64
TILES = 65
HALF = 33
KNOTS = 8192
HALO = 6
UNROLL = 16
LONG = 32
PAIRS = [(0, 0), (0, 1), (0, 2), (1, 1), (1, 2), (2, 2)]
NT = (((1,), (1,)), ((), ()))
NN = (((1,), (0,)), ((), ()))


def moment_row(m, n):
    m, n = min(m, n), max(m, n)
    return {0: n, 4: n + 2, 1: 7 + n, 3: 10 + n, 2: 14 + n}[m]


def parts(value, count):
    out = []
    rest = value
    for _ in range(count - 1):
        top = rest.astype(BF16).astype(F32)
        out.append(top)
        rest = rest - top
    out.append(rest)
    return out


def solve_rows(row):
    factor = {}
    inverse = {}
    for j in range(5):
        for i in range(j, 5):
            running = row(moment_row(j, i)) + (SRC_RIDGE if i == j else 0.0)
            for k in range(j):
                running = running - factor[i, k] * factor[j, k]
            if i == j:
                inverse[j] = 1.0 / jnp.sqrt(running)
            else:
                factor[i, j] = running * inverse[j]
    forward = []
    for i in range(5):
        running = row(moment_row(i, 5))
        for k in range(i):
            running = running - factor[i, k] * forward[k]
        forward.append(running * inverse[i])
    solved = [None] * 5
    for i in reversed(range(5)):
        running = forward[i]
        for k in range(i + 1, 5):
            running = running - factor[k, i] * solved[k]
        solved[i] = running * inverse[i]
    return solved


def kernel(
    design_h, obs_h, wt_h, ph_h, ax_h, sidx_h, kidx_h, cnt_h,
    params_h, att_h, res_h,
    params_o, att_o, res_o, out_sem,
    design, obs, wt, ph, ax, sidx, kidx, cnt, in_sem,
    otlo, otk, bb, wl, ax8, acc, mom, momr, par,
    nloc, nhalf, nsum, nr, npc, nz, nf, nf2,
    rloc, rhalf, rsum, rr, rpc, rz, cp, cb, resid,
    ma_s, ma_r, pa_s, pa_r, nh_s, nh_r, np_s, np_r, nz_s, nz_r, ng_s, ng_r,
    rh_s, rh_r, rp_s, rp_r, rz_s, rz_r, cg_s, cg_r, from_low, from_high,
):
    src = lax.axis_index("src")
    ccd = lax.axis_index("ccd")
    z, y = src // 4, src % 4
    x, core = ccd // 2, ccd % 2
    chip = y * 4 + x
    pid = core * 16 + chip

    def plane(ky, kx, kc):
        return z * 4 + (y + ky) % 4, ((x + kx) % 4) * 2 + (core + kc) % 2

    def along(kz):
        return ((z + kz) % 16) * 4 + y, ccd

    steps16 = [(2, 2), (2, 1), (2, 3), (1, 2), (3, 2), (2, 0), (0, 2), (1, 1), (3, 3), (1, 3), (3, 1), (1, 0), (3, 0), (0, 1), (0, 3)]
    steps32 = [(ky, kx, kc) for ky, kx in steps16 for kc in (1, 0)] + [(0, 0, 1)]
    zsteps = [8, 7, 9, 6, 10, 5, 11, 4, 12, 3, 13, 2, 14, 1, 15]

    loads = []
    held = (sidx, wt, design, obs, ph, ax, kidx)
    for i, (a, b) in enumerate(zip((sidx_h, wt_h, design_h, obs_h, ph_h, ax_h, kidx_h), held)):
        loads.append(pltpu.make_async_copy(a, b, in_sem.at[i]))
        loads[-1].start()

    loads.insert(0, pltpu.make_async_copy(cnt_h, cnt, in_sem.at[7]))
    loads[0].start()

    def send(a, b, ssem, rsem, to):
        copy = pltpu.make_async_remote_copy(
            src_ref=a, dst_ref=b, send_sem=ssem, recv_sem=rsem, device_id=to, device_id_type=MESH
        )
        copy.start()

    def settle(ref, sem):
        pltpu.make_async_copy(ref, ref, sem).wait()

    barrier = pltpu.get_barrier_semaphore()
    for k in steps32:
        pl.semaphore_signal(barrier, inc=1, device_id=plane(*k), device_id_type=MESH)
    for k in (1, 15):
        pl.semaphore_signal(barrier, inc=1, device_id=along(k), device_id_type=MESH)

    def tell():
        pl.semaphore_signal(from_low, inc=1, device_id=along(1), device_id_type=MESH)
        pl.semaphore_signal(from_high, inc=1, device_id=along(15), device_id_type=MESH)

    def heard(last=False):
        pl.semaphore_wait(from_low, 1)
        pl.semaphore_wait(from_high, 1)
        if not last:
            tell()


    lane = lax.broadcasted_iota(jnp.int32, (8, 128), 1)
    lane1 = lax.broadcasted_iota(jnp.int32, (1, 128), 1)
    sub = lax.broadcasted_iota(jnp.int32, (8, 128), 0)
    iota256 = lax.broadcasted_iota(jnp.int32, (256, 128), 0).astype(F32).astype(BF16)
    one, zero = jnp.ones((256, 128), BF16), jnp.zeros((256, 128), BF16)

    def cols(d):
        return pl.ds(pl.multiple_of(d * 128, 128), 128)

    def tall(row, count):
        packed = jnp.broadcast_to(row.astype(F32), (16, 128)).astype(BF16)
        return jnp.concatenate([packed] * count, 0)

    def hot(row, size):
        return jnp.where(iota256[:size] == tall(row, size // 16), one[:size], zero[:size])

    def dot(a, b, dims):
        return lax.dot_general(a, b, dims, precision=lax.Precision.DEFAULT, preferred_element_type=F32)

    for copy in loads[:5]:
        copy.wait()
    acc[...] = jnp.zeros_like(acc)

    def moments_step(t, carry):
        total = None
        for part in range(LONG // 8):
            lefts, hots = [], []
            for b in range(8):
                d = t * LONG + part * 8 + b
                s_row = sidx[pl.ds(d, 1), :]
                hots.append(hot(s_row & 255, 256))
                otlo[:, cols(d)] = hots[-1]
                high = tall(s_row >> 8, 4)
                w = jnp.where(lane1 < cnt[0, d], wt[pl.ds(d, 1), :], 0.0)
                wl[pl.ds(d, 1), :] = w
                e = jnp.concatenate([design[:, cols(d)], jnp.zeros((3, 128), F32)], 0)
                o = jnp.broadcast_to(obs[pl.ds(d, 1), :], (8, 128))
                e0, e1, e2, e3, e4 = [design[i : i + 1, cols(d)] for i in range(5)]
                down = pltpu.roll(e, 2, 0)
                ea = jnp.where(sub < 5, e, jnp.where(sub == 6, e4, o))
                eb = jnp.where(sub < 4, pltpu.roll(e, 7, 0), jnp.where((sub == 5) | (sub == 6), down, o))
                ec = jnp.where(sub < 3, pltpu.roll(e, 6, 0), jnp.where((sub > 3) & (sub < 7), down, o))
                ga = parts(w * ea * jnp.where(sub < 6, e0, e4), 3)
                gb = parts(w * eb * jnp.where(sub < 5, e1, e3), 3)
                gc = parts(w * ec * e2, 3)
                rows = [ga[0], gb[0], ga[1], gb[1], ga[2], gb[2], jnp.where(sub < 4, gc[0], gc[1]), gc[2]]
                stacked = jnp.concatenate(rows, 0).astype(BF16)
                masked = [jnp.where(high == jnp.full((64, 128), h, BF16), stacked, zero[:64]) for h in range(4)]
                lefts.append(jnp.concatenate(masked, 0))
            product = dot(jnp.concatenate(lefts, 1), jnp.concatenate(hots, 1), NT)
            total = product if total is None else total + product
        acc[...] += total
        return carry

    lax.fori_loop(0, BLOCKS // LONG, moments_step, 0)
    for h in range(4):
        v = [acc[64 * h + 8 * i : 64 * h + 8 * i + 8] for i in range(8)]
        tail = v[6] + pltpu.roll(v[6], 4, 0) + v[7]
        total = jnp.concatenate([v[0] + v[2] + v[4], v[1] + v[3] + v[5], tail], 0)
        mom[2 * h] = total[:, :128]
        mom[2 * h + 1] = total[:, 128:]
    pl.semaphore_wait(barrier, len(steps32) + 2)
    tell()
    for k in (4, 5, 3, 2, 6, 7, 1):
        to = (ccd + k) % 8
        send(mom.at[to], momr.at[k - 1], ma_s, ma_r, (src, to))

    for copy in loads[5:]:
        copy.wait()
    u = ph[...]
    rem = 1.0 - u
    sq = u * u
    cu = sq * u
    basis = [
        rem * rem * rem / 6.0,
        (3.0 * cu - 6.0 * sq + 4.0) / 6.0,
        (-3.0 * cu + 3.0 * sq + 3.0 * u + 1.0) / 6.0,
        cu / 6.0,
    ]
    bbid = {}
    for i in range(4):
        bb[i] = basis[i]
    for i in range(4):
        for j in range(i, 4):
            bbid[i, j] = 4 + len(bbid)
            bb[bbid[i, j]] = basis[i] * basis[j]
    ax8[0:3, :] = ax[...]
    ax8[3:4, :] = jnp.zeros((1, KNOTS), F32)
    ax8[4:7, :] = ax[...]
    ax8[7:8, :] = jnp.zeros((1, KNOTS), F32)

    def spread_shift(value, shift):
        lanes = lax.broadcasted_iota(jnp.int32, value.shape, 1)
        turned = pltpu.roll(value, shift, 1)
        return jnp.where(lanes >= shift, turned, 0.0), jnp.where(lanes < shift, turned, 0.0)

    def normal_step(t, carry):
        for pair in range(UNROLL // 2):
            p = t * (UNROLL // 2) + pair
            halves, hots = [], []
            for b in range(2):
                d = 2 * p + b
                own = hot(kidx[pl.ds(d, 1), :], 128)
                hots.append(jnp.concatenate([own, zero[:128]] if b == 0 else [zero[:128], own], 0))
                w = wl[pl.ds(d, 1), :]
                a = [jnp.broadcast_to(ax[i : i + 1, cols(d)], (8, 128)) for i in range(3)]
                wa = [w * a[i] for i in range(3)]
                left = jnp.where(sub < 3, wa[0], jnp.where(sub < 5, wa[1], wa[2]))
                right = jnp.where(sub == 0, a[0], jnp.where((sub == 1) | (sub == 3), a[1], a[2]))
                only = jnp.where(sub < 6, left * right, 0.0)
                tails = [
                    wa[0] * jnp.where(sub == 6, a[0], a[1]),
                    jnp.where(sub == 6, wa[0], wa[1]) * jnp.where(sub == 6, a[2], a[1]),
                    a[2] * jnp.where(sub == 6, wa[1], wa[2]),
                ]

                def term(i, j):
                    return bb[bbid[i, j], pl.ds(d, 1), :]

                last = term(0, 3)
                groups = [jnp.where(sub < 6, only * term(0, o), tails[o] * last) for o in range(3)]
                groups += [only * term(1, 1), only * term(1, 2), only * term(1, 3)]
                groups += [only * term(2, 2), only * term(2, 3), only * term(3, 3)]
                stacked = jnp.concatenate(groups, 0)
                halves.append(jnp.concatenate(parts(stacked, 2), 0).astype(BF16))
            both = jnp.concatenate(halves, 1)
            hot2 = jnp.concatenate(hots, 1)
            otk[p] = hot2
            sums = dot(both, hot2, NT)
            sums = sums[:72] + sums[72:]
            zeros8 = jnp.zeros((8, 128), F32)
            zeros16 = jnp.zeros((16, 128), F32)
            for b in range(2):
                own = sums[:, b * 128 : b * 128 + 128]
                c0, v0 = spread_shift(own[0:24], HALO)
                c1, v1 = spread_shift(own[24:48], HALO + 1)
                c2, v2 = spread_shift(own[48:64], HALO + 2)
                c3, v3 = spread_shift(own[64:72], HALO + 3)
                here = c0 + c1 + jnp.concatenate([c2, zeros8], 0) + jnp.concatenate([c3, zeros16], 0)
                nloc[2 * p + b] = here + carry
                carry = v0 + v1 + jnp.concatenate([v2, zeros8], 0) + jnp.concatenate([v3, zeros16], 0)
        return carry

    mate = (src, x * 2 + (core + 1) % 2)
    empty = jnp.zeros((24, 128), F32)
    nloc[BLOCKS] = empty
    carried = lax.fori_loop(0, 3, lambda t, c: normal_step(t + 1 - core, c), empty)
    nloc[64 - 16 * core] = carried
    send(nloc.at[pl.ds(32 * ((core + 1) % 2), HALF)], nhalf, nh_s, nh_r, mate)
    heard()
    carried = normal_step(3 * core, jnp.where(core == 1, carried, 0.0))
    nloc[16 + 48 * core] = nloc[16 + 48 * core] + carried

    heard()
    settle(momr, ma_r)
    whole = mom[ccd]
    for k in range(7):
        whole = whole + momr[k]
    solved = solve_rows(lambda r: whole[r : r + 1])
    par[ccd] = jnp.concatenate(solved + [jnp.zeros((3, 128), F32)], 0)
    for k in (4, 5, 3, 2, 6, 7, 1):
        send(par.at[ccd], par.at[ccd], pa_s, pa_r, (src, (ccd + k) % 8))
    def pack(halo):
        near = jnp.where(lane < 32, pltpu.roll(halo[1], 16, 1), pltpu.roll(halo[2], 32, 1))
        return jnp.where(lane < 16, halo[0], near)

    settle(nhalf, nh_r)
    for i in range(16):
        for t in range(2):
            tile = nloc[32 * core + 2 * i + t] + nhalf[2 * i + t]
            for g in range(3):
                nsum[i, 3 * t + g] = tile[8 * g : 8 * g + 8]
        if i:
            nsum[i - 1, 6] = pack([nsum[i, g] for g in range(3)])
    tile = nloc[32 * core + 32] + nhalf[32]
    nsum[15, 6] = pack([tile[8 * g : 8 * g + 8] for g in range(3)])

    def to_owner(i):
        ky, kx = steps16[i]
        there = ((y + ky) % 4) * 4 + (x + kx) % 4
        send(nsum.at[there], nr.at[i], np_s, np_r, plane(ky, kx, 0))

    for i in range(15):
        to_owner(i)
    heard()

    settle(par.at[0:7], pa_r)
    heard()
    table = jnp.concatenate([jnp.concatenate([par[2 * h], par[2 * h + 1]], 1) for h in range(4)], 0)
    table = jnp.concatenate(parts(table, 3), 0).astype(BF16)
    upper = sub < 4

    def residual_step(t, carry):
        for part in range(LONG // 8):
            window = otlo[:, pl.ds(pl.multiple_of(t * LONG * 128 + part * 1024, 1024), 1024)]
            picked = dot(table, window, NN)
            picked = picked[0:32] + picked[32:64] + picked[64:96]
            for pair in range(4):
                halves = []
                p = t * (LONG // 2) + part * 4 + pair
                for b in range(2):
                    d = 2 * p + b
                    high = jnp.broadcast_to(sidx[pl.ds(d, 1), :] >> 8, (8, 128))
                    own = picked[:, pair * 256 + b * 128 : pair * 256 + b * 128 + 128]
                    chosen = own[0:8]
                    for h in range(1, 4):
                        chosen = jnp.where(high == h, own[8 * h : 8 * h + 8], chosen)
                    fitted = jnp.sum(chosen[0:5] * design[:, cols(d)], 0, keepdims=True)
                    r = jnp.where(lane1 < cnt[0, d], obs[pl.ds(d, 1), :] - fitted, 0.0)
                    resid[pl.ds(d, 1), :] = r
                    wr = jnp.broadcast_to(wl[pl.ds(d, 1), :] * r, (8, 128))
                    a = ax8[:, cols(d)] * wr
                    pair01 = a * jnp.where(upper, bb[0, pl.ds(d, 1), :], bb[1, pl.ds(d, 1), :])
                    pair23 = a * jnp.where(upper, bb[2, pl.ds(d, 1), :], bb[3, pl.ds(d, 1), :])
                    stacked = jnp.concatenate([pair01, pair23], 0)
                    halves.append(jnp.concatenate(parts(stacked, 3), 0).astype(BF16))
                both = jnp.concatenate(halves, 1)
                sums = dot(both, otk[p], NT)
                sums = sums[0:16] + sums[16:32] + sums[32:48]
                for b in range(2):
                    here = carry
                    over = jnp.zeros((8, 128), F32)
                    for g in range(2):
                        value = sums[8 * g : 8 * g + 8, b * 128 : b * 128 + 128]
                        first, second = HALO + 2 * g, HALO + 2 * g + 1
                        turned = jnp.where(upper, pltpu.roll(value, first, 1), pltpu.roll(value, second, 1))
                        limit = jnp.where(upper, first, second)
                        here = here + jnp.where(lane >= limit, turned, 0.0)
                        over = over + jnp.where(lane < limit, turned, 0.0)
                    folded = here + pltpu.roll(here, 4, 0)
                    rloc[2 * p + b] = folded[0:4]
                    carry = over
        return carry

    last = lax.fori_loop(0, BLOCKS // LONG, residual_step, jnp.zeros((8, 128), F32))
    last = last + pltpu.roll(last, 4, 0)
    rloc[BLOCKS] = last[0:4]

    send(rloc.at[pl.ds(32 * ((core + 1) % 2), HALF)], rhalf, rh_s, rh_r, mate)
    heard()
    for c in range(8):
        params_o[:, c * 128 : (c + 1) * 128] = par[c, 0:5]
    params_out = pltpu.make_async_copy(params_o, params_h, out_sem.at[0])
    params_out.start()
    settle(rhalf, rh_r)
    for i in range(16):
        for t in range(2):
            rsum[i, t] = rloc[32 * core + 2 * i + t] + rhalf[2 * i + t]
        rsum[i, 2] = rloc[32 * core + 2 * i + 2] + rhalf[2 * i + 2]
    for i, (ky, kx) in enumerate(steps16):
        there = ((y + ky) % 4) * 4 + (x + kx) % 4
        send(rsum.at[there], rr.at[i], rp_s, rp_r, plane(ky, kx, 0))

    heard()
    settle(nr, np_r)
    for g in range(7):
        total = nsum[chip, g]
        for i in range(15):
            total = total + nr[i, g]
        npc[g] = total
    heard(last=True)
    mine, half = z % 8, z // 8
    is_owner = mine < 7
    for g in range(7):
        owner = g + 8 * ((((z + 16 - g) % 16 + 4) // 8) % 2)
        slot = (z + 20 - owner) % 16

        @pl.when(owner != z)
        def _(g=g, owner=owner, slot=slot):
            pltpu.make_async_remote_copy(
                src_ref=npc.at[g], dst_ref=nz.at[slot], send_sem=nz_s, recv_sem=nz_r,
                device_id=(owner * 4 + y, ccd), device_id_type=MESH,
            ).start()

    settle(rr, rp_r)
    rows = []
    for t in range(3):
        total = rsum[chip, t]
        for i in range(15):
            total = total + rr[i, t]
        rows.append(total)
    low = jnp.concatenate(rows[:2], 0)
    edge = jnp.where(lane1 < 16, rows[2][0:1], jnp.where(lane1 < 32, pltpu.roll(rows[2], 16, 1)[1:2], pltpu.roll(rows[2], 32, 1)[2:3]))
    rpc[...] = jnp.where((sub == 3) | (sub == 7), jnp.broadcast_to(edge, (8, 128)), low)
    for kz in zsteps:
        send(rpc, rz.at[kz - 1], rz_s, rz_r, along(kz))

    @pl.when(is_owner)
    def _():
        total = npc[mine]
        settle(nz.at[0:7], nz_r)
        for k in (0, 1, 2, 3, 5, 6, 7):
            total = total + nz[k]
        nf2[7 * half + mine] = total
        for k in zsteps:
            pltpu.make_async_remote_copy(
                src_ref=nf2.at[7 * half + mine], dst_ref=nf2.at[7 * half + mine], send_sem=ng_s, recv_sem=ng_r,
                device_id=along(k), device_id_type=MESH,
            ).start()

    settle(rz, rz_r)
    flat = rpc[...]
    for i in range(15):
        flat = flat + rz[i]
    @pl.when(is_owner)
    def _():
        settle(nf2.at[0:13], ng_r)

    @pl.when(jnp.logical_not(is_owner))
    def _():
        settle(nf2, ng_r)

    nf[...] = nf2[0:7] + nf2[7:14]

    def wide(pieces):
        return jnp.concatenate([jnp.broadcast_to(piece, (8, 128)) for piece in pieces], 1)

    edges = [nf[6], pltpu.roll(nf[6], 112, 1), pltpu.roll(nf[6], 96, 1)]

    def band(o, pair):
        g, s = (o, pair) if o < 3 else (pair // 2, 6 + pair % 2)
        return wide([nf[g, s : s + 1], nf[3 + g, s : s + 1], edges[g][s : s + 1]])

    bands = [{} for _ in range(4)]
    for o in range(4):
        for p, (a, b) in enumerate(PAIRS):
            bands[o][a, b] = bands[o][b, a] = band(o, p)
    inside = lax.broadcasted_iota(jnp.int32, (8, 384), 1) < jnp.minimum(KNOTS + HALO - 256 * pid, 256 + 2 * HALO)
    shifted = [flat, pltpu.roll(flat, 112, 1), pltpu.roll(flat, 96, 1)]
    rhs = [wide([flat[i : i + 1], flat[4 + i : 5 + i], shifted[i][3:4]]) for i in range(3)]
    scale = [RELAX / (ATT_RIDGE + bands[0][i, i]) for i in range(3)]
    coef = [jnp.where(inside, rhs[i] * scale[i], 0.0) for i in range(3)]
    for _ in range(1, SWEEPS):
        ahead = [[pltpu.roll(coef[i], 384 - o, 1) for i in range(3)] for o in range(1, 4)]
        fresh = []
        for i in range(3):
            product = coef[i] * ATT_RIDGE
            for k in range(3):
                product = product + bands[0][i, k] * coef[k]
            for o in range(1, 4):
                back = bands[o][i, 0] * coef[0] + bands[o][i, 1] * coef[1] + bands[o][i, 2] * coef[2]
                product = product + pltpu.roll(back, o, 1)
                for k in range(3):
                    product = product + bands[o][i, k] * ahead[o - 1][k]
            fresh.append(jnp.where(inside, coef[i] + scale[i] * (rhs[i] - product), 0.0))
        coef = fresh
    cp[:, 3:4, :] = jnp.zeros((2, 1, 128), F32)
    for i in range(3):
        moved = pltpu.roll(coef[i], 384 - HALO, 1)
        for t in range(2):
            cp[t, i : i + 1] = moved[0:1, t * 128 : (t + 1) * 128]
    for i, k in enumerate(steps32):
        send(cp, cb.at[pl.ds(2 * pid, 2)], cg_s, cg_r, plane(*k))
    for t in range(2):
        cb[2 * pid + t] = cp[t]
    cb[BLOCKS] = jnp.zeros((4, 128), F32)
    settle(cb.at[0:62], cg_r)
    att_o[...] = cb[src][0:3]
    att_out = pltpu.make_async_copy(att_o, att_h, out_sem.at[1])
    att_out.start()

    def final_step(t, carry):
        for pair in range(LONG // 2):
            p = t * (LONG // 2) + pair
            halves = []
            for b in range(2):
                d = 2 * p + b
                now = jnp.concatenate([cb[d], cb[d + 1]], 0)
                turned = [now] + [pltpu.roll(now, 128 - j, 1) for j in range(1, 4)]
                flip = [pltpu.roll(v, 4, 0) for v in turned]
                pair01 = jnp.where(
                    upper, now, jnp.where(lane < 127, flip[1], turned[1])
                )
                pair23 = jnp.where(
                    upper,
                    jnp.where(lane < 126, turned[2], flip[2]),
                    jnp.where(lane < 125, flip[3], turned[3]),
                )
                stacked = jnp.concatenate([pair01, pair23], 0)
                halves.append(jnp.concatenate(parts(stacked, 3), 0).astype(BF16))
            both = jnp.concatenate(halves, 1)
            picked = dot(both, otk[p], NN)
            picked = picked[0:16] + picked[16:32] + picked[32:48]
            for b in range(2):
                d = 2 * p + b
                own = picked[:, b * 128 : b * 128 + 128]
                b01 = jnp.where(upper, bb[0, pl.ds(d, 1), :], bb[1, pl.ds(d, 1), :])
                b23 = jnp.where(upper, bb[2, pl.ds(d, 1), :], bb[3, pl.ds(d, 1), :])
                terms = ax8[:, cols(d)] * (own[0:8] * b01 + own[8:16] * b23)
                predicted = jnp.sum(terms, 0, keepdims=True)
                res_o[pl.ds(d, 1), :] = jnp.where(
                    lane1 < cnt[0, d], resid[pl.ds(d, 1), :] - predicted, 0.0
                )
        return carry

    lax.fori_loop(0, BLOCKS // LONG, final_step, 0)
    res_out = pltpu.make_async_copy(res_o, res_h, out_sem.at[2])
    res_out.start()

    settle(momr, ma_s)
    settle(par.at[0:7], pa_s)
    settle(nhalf, nh_s)
    settle(nr, np_s)
    settle(rhalf, rh_s)
    settle(rr, rp_s)
    settle(rz, rz_s)
    settle(cb.at[0:62], cg_s)

    @pl.when(is_owner)
    def _():
        settle(nz.at[0:6], nz_s)
        settle(rz, ng_s)

    @pl.when(jnp.logical_not(is_owner))
    def _():
        settle(nz.at[0:7], nz_s)

    for copy in (params_out, att_out, res_out):
        copy.wait()


def write_out(params_i, att_i, res_i, params_o, att_o, res_o, params, attitude, residual, sems):
    held = (params, attitude, residual)
    inward = [pltpu.make_async_copy(a, b, sems.at[i]) for i, (a, b) in enumerate(zip((params_i, att_i, res_i), held))]
    outward = [pltpu.make_async_copy(a, b, sems.at[i + 3]) for i, (a, b) in enumerate(zip(held, (params_o, att_o, res_o)))]
    for copy in inward:
        copy.start()
    for there, back in zip(inward, outward):
        there.wait()
        back.start()
    for copy in outward:
        copy.wait()


def on_device(design, observed, weight, phase_frac, axis_factors, source_index, knot_index, counts):
    dma = pltpu.SemaphoreType.DMA
    vm = lambda *shape: pltpu.VMEM(shape, F32)
    square = lambda v: v.reshape(64, 128)
    params, attitude, residual = pl.pallas_call(
        kernel,
        out_shape=(
            jax.ShapeDtypeStruct((5, 1024), F32),
            jax.ShapeDtypeStruct((3, 128), F32),
            jax.ShapeDtypeStruct((64, 128), F32),
        ),
        in_specs=[pl.BlockSpec(memory_space=pl.ANY)] * 8,
        out_specs=(pl.BlockSpec(memory_space=pl.ANY),) * 3,
        scratch_shapes=[
            vm(5, 1024), vm(3, 128), vm(64, 128), dma((3,)),
            vm(5, 8192), vm(64, 128), vm(64, 128), vm(64, 128), vm(3, 8192),
            pltpu.VMEM((64, 128), jnp.int32), pltpu.VMEM((64, 128), jnp.int32), pltpu.SMEM((1, 64), jnp.int32), dma((8,)),
            pltpu.VMEM((256, 8192), BF16),
            pltpu.VMEM((32, 256, 256), BF16),
            vm(14, 64, 128), vm(64, 128), vm(8, 8192),
            vm(256, 256), vm(8, 24, 128), vm(7, 24, 128), vm(8, 8, 128),
            vm(TILES, 24, 128), vm(HALF, 24, 128), vm(16, 7, 8, 128), vm(15, 7, 8, 128),
            vm(7, 8, 128), vm(8, 8, 128), vm(7, 8, 128), vm(14, 8, 128),
            vm(TILES, 4, 128), vm(HALF, 4, 128), vm(16, 3, 4, 128), vm(15, 3, 4, 128),
            vm(8, 128), vm(15, 8, 128), vm(2, 4, 128), vm(TILES, 4, 128), vm(64, 128),
        ]
        + [dma] * 20
        + [pltpu.SemaphoreType.REGULAR] * 2,
        compiler_params=pltpu.CompilerParams(
            collective_id=0, has_side_effects=True, vmem_limit_bytes=60 * 1024 * 1024
        ),
    )(
        design, square(observed), square(weight), square(phase_frac), axis_factors,
        square(source_index), square(knot_index), counts.reshape(1, 64),
    )
    anywhere = pl.BlockSpec(memory_space=pl.ANY)
    params, attitude, residual = pl.pallas_call(
        write_out,
        out_shape=(
            jax.ShapeDtypeStruct((5, 1024), F32),
            jax.ShapeDtypeStruct((3, 128), F32),
            jax.ShapeDtypeStruct((64, 128), F32),
        ),
        in_specs=[anywhere] * 3,
        out_specs=(anywhere,) * 3,
        scratch_shapes=[vm(5, 1024), vm(3, 128), vm(64, 128), dma((6,))],
        compiler_params=pltpu.CompilerParams(vmem_limit_bytes=60 * 1024 * 1024),
    )(params, attitude, residual)
    return params, attitude, residual.reshape(8192)


def solution(mesh):
    rows = P(("src", "ccd"))
    wide = P(None, ("src", "ccd"))
    in_specs = (wide, rows, rows, rows, wide, rows, rows, P("src", "ccd", None))
    out_specs = (P(None, "src"), P(None, "src"), rows)
    return jax.shard_map(on_device, mesh=mesh, in_specs=in_specs, out_specs=out_specs, check_vma=False)
```

```python
import functools

import jax
import jax.numpy as jnp
from jax import lax
from jax.experimental import pallas as pl
from jax.experimental.pallas import tpu as pltpu
from jax.sharding import PartitionSpec as P

F32 = jnp.float32
BF16 = jnp.bfloat16
MESH = pl.DeviceIdType.MESH
SRC_RIDGE = 1.0
ATT_RIDGE = 1.0
RELAX = 0.15
SWEEPS = 3
BLOCKS = 64
TILES = 65
HALF = 33
KNOTS = 8192
HALO = 6
UNROLL = 16
LONG = 32
PAIRS = [(0, 0), (0, 1), (0, 2), (1, 1), (1, 2), (2, 2)]
NT = (((1,), (1,)), ((), ()))
NN = (((1,), (0,)), ((), ()))


def moment_row(m, n):
    m, n = min(m, n), max(m, n)
    return {0: n, 4: n + 2, 1: 7 + n, 3: 10 + n, 2: 14 + n}[m]


def parts(value, count):
    out = []
    rest = value
    for _ in range(count - 1):
        top = rest.astype(BF16).astype(F32)
        out.append(top)
        rest = rest - top
    out.append(rest)
    return out


def solve_rows(row):
    factor = {}
    inverse = {}
    for j in range(5):
        for i in range(j, 5):
            running = row(moment_row(j, i)) + (SRC_RIDGE if i == j else 0.0)
            for k in range(j):
                running = running - factor[i, k] * factor[j, k]
            if i == j:
                inverse[j] = 1.0 / jnp.sqrt(running)
            else:
                factor[i, j] = running * inverse[j]
    forward = []
    for i in range(5):
        running = row(moment_row(i, 5))
        for k in range(i):
            running = running - factor[i, k] * forward[k]
        forward.append(running * inverse[i])
    solved = [None] * 5
    for i in reversed(range(5)):
        running = forward[i]
        for k in range(i + 1, 5):
            running = running - factor[k, i] * solved[k]
        solved[i] = running * inverse[i]
    return solved


def kernel(
    design_h, obs_h, wt_h, ph_h, ax_h, sidx_h, kidx_h, cnt_h,
    params_h, att_h, res_h,
    params_o, att_o, res_o, out_sem,
    design, obs, wt, ph, ax, sidx, kidx, cnt, in_sem,
    otlo, otk, bb, wl, ax8, acc, mom, momr, par,
    nloc, nhalf, nsum, nr, npc, nz, nf, nf2,
    rloc, rhalf, rsum, rr, rpc, rz, cp, cb, resid,
    ma_s, ma_r, pa_s, pa_r, nh_s, nh_r, np_s, np_r, nz_s, nz_r, ng_s, ng_r,
    rh_s, rh_r, rp_s, rp_r, rz_s, rz_r, cg_s, cg_r, from_low, from_high,
):
    src = lax.axis_index("src")
    ccd = lax.axis_index("ccd")
    z, y = src // 4, src % 4
    x, core = ccd // 2, ccd % 2
    chip = y * 4 + x
    pid = core * 16 + chip

    def plane(ky, kx, kc):
        return z * 4 + (y + ky) % 4, ((x + kx) % 4) * 2 + (core + kc) % 2

    def along(kz):
        return ((z + kz) % 16) * 4 + y, ccd

    steps16 = [(2, 2), (2, 1), (2, 3), (1, 2), (3, 2), (2, 0), (0, 2), (1, 1), (3, 3), (1, 3), (3, 1), (1, 0), (3, 0), (0, 1), (0, 3)]
    steps32 = [(ky, kx, kc) for ky, kx in steps16 for kc in (1, 0)] + [(0, 0, 1)]
    zsteps = [8, 7, 9, 6, 10, 5, 11, 4, 12, 3, 13, 2, 14, 1, 15]

    loads = []
    held = (sidx, wt, design, obs, ph, ax, kidx)
    for i, (a, b) in enumerate(zip((sidx_h, wt_h, design_h, obs_h, ph_h, ax_h, kidx_h), held)):
        loads.append(pltpu.make_async_copy(a, b, in_sem.at[i]))
        loads[-1].start()

    loads.insert(0, pltpu.make_async_copy(cnt_h, cnt, in_sem.at[7]))
    loads[0].start()

    def send(a, b, ssem, rsem, to):
        copy = pltpu.make_async_remote_copy(
            src_ref=a, dst_ref=b, send_sem=ssem, recv_sem=rsem, device_id=to, device_id_type=MESH
        )
        copy.start()

    def settle(ref, sem):
        pltpu.make_async_copy(ref, ref, sem).wait()

    barrier = pltpu.get_barrier_semaphore()
    for k in steps32:
        pl.semaphore_signal(barrier, inc=1, device_id=plane(*k), device_id_type=MESH)
    for k in (1, 15):
        pl.semaphore_signal(barrier, inc=1, device_id=along(k), device_id_type=MESH)

    def tell():
        pl.semaphore_signal(from_low, inc=1, device_id=along(1), device_id_type=MESH)
        pl.semaphore_signal(from_high, inc=1, device_id=along(15), device_id_type=MESH)

    def heard(last=False):
        pl.semaphore_wait(from_low, 1)
        pl.semaphore_wait(from_high, 1)
        if not last:
            tell()


    lane = lax.broadcasted_iota(jnp.int32, (8, 128), 1)
    lane1 = lax.broadcasted_iota(jnp.int32, (1, 128), 1)
    sub = lax.broadcasted_iota(jnp.int32, (8, 128), 0)
    iota256 = lax.broadcasted_iota(jnp.int32, (256, 128), 0).astype(F32).astype(BF16)
    one, zero = jnp.ones((256, 128), BF16), jnp.zeros((256, 128), BF16)

    def cols(d):
        return pl.ds(pl.multiple_of(d * 128, 128), 128)

    def tall(row, count):
        packed = jnp.broadcast_to(row.astype(F32), (16, 128)).astype(BF16)
        return jnp.concatenate([packed] * count, 0)

    def hot(row, size):
        return jnp.where(iota256[:size] == tall(row, size // 16), one[:size], zero[:size])

    def dot(a, b, dims):
        return lax.dot_general(a, b, dims, precision=lax.Precision.DEFAULT, preferred_element_type=F32)

    for copy in loads[:5]:
        copy.wait()
    acc[...] = jnp.zeros_like(acc)

    def moments_step(t, carry):
        total = None
        for part in range(LONG // 8):
            lefts, hots = [], []
            for b in range(8):
                d = t * LONG + part * 8 + b
                s_row = sidx[pl.ds(d, 1), :]
                hots.append(hot(s_row & 255, 256))
                otlo[:, cols(d)] = hots[-1]
                high = tall(s_row >> 8, 4)
                w = jnp.where(lane1 < cnt[0, d], wt[pl.ds(d, 1), :], 0.0)
                wl[pl.ds(d, 1), :] = w
                e = jnp.concatenate([design[:, cols(d)], jnp.zeros((3, 128), F32)], 0)
                o = jnp.broadcast_to(obs[pl.ds(d, 1), :], (8, 128))
                e0, e1, e2, e3, e4 = [design[i : i + 1, cols(d)] for i in range(5)]
                down = pltpu.roll(e, 2, 0)
                ea = jnp.where(sub < 5, e, jnp.where(sub == 6, e4, o))
                eb = jnp.where(sub < 4, pltpu.roll(e, 7, 0), jnp.where((sub == 5) | (sub == 6), down, o))
                ec = jnp.where(sub < 3, pltpu.roll(e, 6, 0), jnp.where((sub > 3) & (sub < 7), down, o))
                ga = parts(w * ea * jnp.where(sub < 6, e0, e4), 3)
                gb = parts(w * eb * jnp.where(sub < 5, e1, e3), 3)
                gc = parts(w * ec * e2, 3)
                rows = [ga[0], gb[0], ga[1], gb[1], ga[2], gb[2], jnp.where(sub < 4, gc[0], gc[1]), gc[2]]
                stacked = jnp.concatenate(rows, 0).astype(BF16)
                masked = [jnp.where(high == jnp.full((64, 128), h, BF16), stacked, zero[:64]) for h in range(4)]
                lefts.append(jnp.concatenate(masked, 0))
            product = dot(jnp.concatenate(lefts, 1), jnp.concatenate(hots, 1), NT)
            total = product if total is None else total + product
        acc[...] += total
        return carry

    lax.fori_loop(0, BLOCKS // LONG, moments_step, 0)
    for h in range(4):
        v = [acc[64 * h + 8 * i : 64 * h + 8 * i + 8] for i in range(8)]
        tail = v[6] + pltpu.roll(v[6], 4, 0) + v[7]
        total = jnp.concatenate([v[0] + v[2] + v[4], v[1] + v[3] + v[5], tail], 0)
        mom[2 * h] = total[:, :128]
        mom[2 * h + 1] = total[:, 128:]
    pl.semaphore_wait(barrier, len(steps32) + 2)
    tell()
    for k in (4, 5, 3, 2, 6, 7, 1):
        to = (ccd + k) % 8
        send(mom.at[to], momr.at[k - 1], ma_s, ma_r, (src, to))

    for copy in loads[5:]:
        copy.wait()
    u = ph[...]
    rem = 1.0 - u
    sq = u * u
    cu = sq * u
    basis = [
        rem * rem * rem / 6.0,
        (3.0 * cu - 6.0 * sq + 4.0) / 6.0,
        (-3.0 * cu + 3.0 * sq + 3.0 * u + 1.0) / 6.0,
        cu / 6.0,
    ]
    bbid = {}
    for i in range(4):
        bb[i] = basis[i]
    for i in range(4):
        for j in range(i, 4):
            bbid[i, j] = 4 + len(bbid)
            bb[bbid[i, j]] = basis[i] * basis[j]
    ax8[0:3, :] = ax[...]
    ax8[3:4, :] = jnp.zeros((1, KNOTS), F32)
    ax8[4:7, :] = ax[...]
    ax8[7:8, :] = jnp.zeros((1, KNOTS), F32)

    def spread_shift(value, shift):
        lanes = lax.broadcasted_iota(jnp.int32, value.shape, 1)
        turned = pltpu.roll(value, shift, 1)
        return jnp.where(lanes >= shift, turned, 0.0), jnp.where(lanes < shift, turned, 0.0)

    def normal_step(t, carry):
        for pair in range(UNROLL // 2):
            p = t * (UNROLL // 2) + pair
            halves, hots = [], []
            for b in range(2):
                d = 2 * p + b
                own = hot(kidx[pl.ds(d, 1), :], 128)
                hots.append(jnp.concatenate([own, zero[:128]] if b == 0 else [zero[:128], own], 0))
                w = wl[pl.ds(d, 1), :]
                a = [jnp.broadcast_to(ax[i : i + 1, cols(d)], (8, 128)) for i in range(3)]
                wa = [w * a[i] for i in range(3)]
                left = jnp.where(sub < 3, wa[0], jnp.where(sub < 5, wa[1], wa[2]))
                right = jnp.where(sub == 0, a[0], jnp.where((sub == 1) | (sub == 3), a[1], a[2]))
                only = jnp.where(sub < 6, left * right, 0.0)
                tails = [
                    wa[0] * jnp.where(sub == 6, a[0], a[1]),
                    jnp.where(sub == 6, wa[0], wa[1]) * jnp.where(sub == 6, a[2], a[1]),
                    a[2] * jnp.where(sub == 6, wa[1], wa[2]),
                ]

                def term(i, j):
                    return bb[bbid[i, j], pl.ds(d, 1), :]

                last = term(0, 3)
                groups = [jnp.where(sub < 6, only * term(0, o), tails[o] * last) for o in range(3)]
                groups += [only * term(1, 1), only * term(1, 2), only * term(1, 3)]
                groups += [only * term(2, 2), only * term(2, 3), only * term(3, 3)]
                stacked = jnp.concatenate(groups, 0)
                halves.append(jnp.concatenate(parts(stacked, 2), 0).astype(BF16))
            both = jnp.concatenate(halves, 1)
            hot2 = jnp.concatenate(hots, 1)
            otk[p] = hot2
            sums = dot(both, hot2, NT)
            sums = sums[:72] + sums[72:]
            zeros8 = jnp.zeros((8, 128), F32)
            zeros16 = jnp.zeros((16, 128), F32)
            for b in range(2):
                own = sums[:, b * 128 : b * 128 + 128]
                c0, v0 = spread_shift(own[0:24], HALO)
                c1, v1 = spread_shift(own[24:48], HALO + 1)
                c2, v2 = spread_shift(own[48:64], HALO + 2)
                c3, v3 = spread_shift(own[64:72], HALO + 3)
                here = c0 + c1 + jnp.concatenate([c2, zeros8], 0) + jnp.concatenate([c3, zeros16], 0)
                nloc[2 * p + b] = here + carry
                carry = v0 + v1 + jnp.concatenate([v2, zeros8], 0) + jnp.concatenate([v3, zeros16], 0)
        return carry

    mate = (src, x * 2 + (core + 1) % 2)
    empty = jnp.zeros((24, 128), F32)
    nloc[BLOCKS] = empty
    carried = lax.fori_loop(0, 3, lambda t, c: normal_step(t + 1 - core, c), empty)
    nloc[64 - 16 * core] = carried
    send(nloc.at[pl.ds(32 * ((core + 1) % 2), HALF)], nhalf, nh_s, nh_r, mate)
    heard()
    carried = normal_step(3 * core, jnp.where(core == 1, carried, 0.0))
    nloc[16 + 48 * core] = nloc[16 + 48 * core] + carried

    heard()
    settle(momr, ma_r)
    whole = mom[ccd]
    for k in range(7):
        whole = whole + momr[k]
    solved = solve_rows(lambda r: whole[r : r + 1])
    par[ccd] = jnp.concatenate(solved + [jnp.zeros((3, 128), F32)], 0)
    for k in (4, 5, 3, 2, 6, 7, 1):
        send(par.at[ccd], par.at[ccd], pa_s, pa_r, (src, (ccd + k) % 8))
    def pack(halo):
        near = jnp.where(lane < 32, pltpu.roll(halo[1], 16, 1), pltpu.roll(halo[2], 32, 1))
        return jnp.where(lane < 16, halo[0], near)

    settle(nhalf, nh_r)
    for i in range(16):
        for t in range(2):
            tile = nloc[32 * core + 2 * i + t] + nhalf[2 * i + t]
            for g in range(3):
                nsum[i, 3 * t + g] = tile[8 * g : 8 * g + 8]
        if i:
            nsum[i - 1, 6] = pack([nsum[i, g] for g in range(3)])
    tile = nloc[32 * core + 32] + nhalf[32]
    nsum[15, 6] = pack([tile[8 * g : 8 * g + 8] for g in range(3)])

    def to_owner(i):
        ky, kx = steps16[i]
        there = ((y + ky) % 4) * 4 + (x + kx) % 4
        send(nsum.at[there], nr.at[i], np_s, np_r, plane(ky, kx, 0))

    for i in range(15):
        to_owner(i)
    heard()
    heard()

    settle(par.at[0:7], pa_r)
    heard()
    table = jnp.concatenate([jnp.concatenate([par[2 * h], par[2 * h + 1]], 1) for h in range(4)], 0)
    table = jnp.concatenate(parts(table, 3), 0).astype(BF16)
    upper = sub < 4

    def residual_step(t, carry):
        for part in range(LONG // 8):
            window = otlo[:, pl.ds(pl.multiple_of(t * LONG * 128 + part * 1024, 1024), 1024)]
            picked = dot(table, window, NN)
            picked = picked[0:32] + picked[32:64] + picked[64:96]
            for pair in range(4):
                halves = []
                p = t * (LONG // 2) + part * 4 + pair
                for b in range(2):
                    d = 2 * p + b
                    high = jnp.broadcast_to(sidx[pl.ds(d, 1), :] >> 8, (8, 128))
                    own = picked[:, pair * 256 + b * 128 : pair * 256 + b * 128 + 128]
                    chosen = own[0:8]
                    for h in range(1, 4):
                        chosen = jnp.where(high == h, own[8 * h : 8 * h + 8], chosen)
                    fitted = jnp.sum(chosen[0:5] * design[:, cols(d)], 0, keepdims=True)
                    r = jnp.where(lane1 < cnt[0, d], obs[pl.ds(d, 1), :] - fitted, 0.0)
                    resid[pl.ds(d, 1), :] = r
                    wr = jnp.broadcast_to(wl[pl.ds(d, 1), :] * r, (8, 128))
                    a = ax8[:, cols(d)] * wr
                    pair01 = a * jnp.where(upper, bb[0, pl.ds(d, 1), :], bb[1, pl.ds(d, 1), :])
                    pair23 = a * jnp.where(upper, bb[2, pl.ds(d, 1), :], bb[3, pl.ds(d, 1), :])
                    stacked = jnp.concatenate([pair01, pair23], 0)
                    halves.append(jnp.concatenate(parts(stacked, 3), 0).astype(BF16))
                both = jnp.concatenate(halves, 1)
                sums = dot(both, otk[p], NT)
                sums = sums[0:16] + sums[16:32] + sums[32:48]
                for b in range(2):
                    here = carry
                    over = jnp.zeros((8, 128), F32)
                    for g in range(2):
                        value = sums[8 * g : 8 * g + 8, b * 128 : b * 128 + 128]
                        first, second = HALO + 2 * g, HALO + 2 * g + 1
                        turned = jnp.where(upper, pltpu.roll(value, first, 1), pltpu.roll(value, second, 1))
                        limit = jnp.where(upper, first, second)
                        here = here + jnp.where(lane >= limit, turned, 0.0)
                        over = over + jnp.where(lane < limit, turned, 0.0)
                    folded = here + pltpu.roll(here, 4, 0)
                    rloc[2 * p + b] = folded[0:4]
                    carry = over
        return carry

    last = lax.fori_loop(0, BLOCKS // LONG, residual_step, jnp.zeros((8, 128), F32))
    last = last + pltpu.roll(last, 4, 0)
    rloc[BLOCKS] = last[0:4]

    send(rloc.at[pl.ds(32 * ((core + 1) % 2), HALF)], rhalf, rh_s, rh_r, mate)
    heard()
    for c in range(8):
        params_o[:, c * 128 : (c + 1) * 128] = par[c, 0:5]
    params_out = pltpu.make_async_copy(params_o, params_h, out_sem.at[0])
    params_out.start()
    settle(rhalf, rh_r)
    for i in range(16):
        for t in range(2):
            rsum[i, t] = rloc[32 * core + 2 * i + t] + rhalf[2 * i + t]
        rsum[i, 2] = rloc[32 * core + 2 * i + 2] + rhalf[2 * i + 2]
    for i, (ky, kx) in enumerate(steps16):
        there = ((y + ky) % 4) * 4 + (x + kx) % 4
        send(rsum.at[there], rr.at[i], rp_s, rp_r, plane(ky, kx, 0))

    heard(last=True)
    settle(nr, np_r)
    for g in range(7):
        total = nsum[chip, g]
        for i in range(15):
            total = total + nr[i, g]
        npc[g] = total
    mine, half = z % 8, z // 8
    is_owner = mine < 7
    for g in range(7):
        owner = g + 8 * ((((z + 16 - g) % 16 + 4) // 8) % 2)
        slot = (z + 20 - owner) % 16

        @pl.when(owner != z)
        def _(g=g, owner=owner, slot=slot):
            pltpu.make_async_remote_copy(
                src_ref=npc.at[g], dst_ref=nz.at[slot], send_sem=nz_s, recv_sem=nz_r,
                device_id=(owner * 4 + y, ccd), device_id_type=MESH,
            ).start()

    settle(rr, rp_r)
    rows = []
    for t in range(3):
        total = rsum[chip, t]
        for i in range(15):
            total = total + rr[i, t]
        rows.append(total)
    low = jnp.concatenate(rows[:2], 0)
    edge = jnp.where(lane1 < 16, rows[2][0:1], jnp.where(lane1 < 32, pltpu.roll(rows[2], 16, 1)[1:2], pltpu.roll(rows[2], 32, 1)[2:3]))
    rpc[...] = jnp.where((sub == 3) | (sub == 7), jnp.broadcast_to(edge, (8, 128)), low)
    for kz in zsteps:
        send(rpc, rz.at[kz - 1], rz_s, rz_r, along(kz))

    @pl.when(is_owner)
    def _():
        total = npc[mine]
        settle(nz.at[0:7], nz_r)
        for k in (0, 1, 2, 3, 5, 6, 7):
            total = total + nz[k]
        nf2[7 * half + mine] = total
        for k in zsteps:
            pltpu.make_async_remote_copy(
                src_ref=nf2.at[7 * half + mine], dst_ref=nf2.at[7 * half + mine], send_sem=ng_s, recv_sem=ng_r,
                device_id=along(k), device_id_type=MESH,
            ).start()

    settle(rz, rz_r)
    flat = rpc[...]
    for i in range(15):
        flat = flat + rz[i]
    @pl.when(is_owner)
    def _():
        settle(nf2.at[0:13], ng_r)

    @pl.when(jnp.logical_not(is_owner))
    def _():
        settle(nf2, ng_r)

    nf[...] = nf2[0:7] + nf2[7:14]

    def wide(pieces):
        return jnp.concatenate([jnp.broadcast_to(piece, (8, 128)) for piece in pieces], 1)

    edges = [nf[6], pltpu.roll(nf[6], 112, 1), pltpu.roll(nf[6], 96, 1)]

    def band(o, pair):
        g, s = (o, pair) if o < 3 else (pair // 2, 6 + pair % 2)
        return wide([nf[g, s : s + 1], nf[3 + g, s : s + 1], edges[g][s : s + 1]])

    bands = [{} for _ in range(4)]
    for o in range(4):
        for p, (a, b) in enumerate(PAIRS):
            bands[o][a, b] = bands[o][b, a] = band(o, p)
    inside = lax.broadcasted_iota(jnp.int32, (8, 384), 1) < jnp.minimum(KNOTS + HALO - 256 * pid, 256 + 2 * HALO)
    shifted = [flat, pltpu.roll(flat, 112, 1), pltpu.roll(flat, 96, 1)]
    rhs = [wide([flat[i : i + 1], flat[4 + i : 5 + i], shifted[i][3:4]]) for i in range(3)]
    scale = [RELAX / (ATT_RIDGE + bands[0][i, i]) for i in range(3)]
    coef = [jnp.where(inside, rhs[i] * scale[i], 0.0) for i in range(3)]
    for _ in range(1, SWEEPS):
        ahead = [[pltpu.roll(coef[i], 384 - o, 1) for i in range(3)] for o in range(1, 4)]
        fresh = []
        for i in range(3):
            product = coef[i] * ATT_RIDGE
            for k in range(3):
                product = product + bands[0][i, k] * coef[k]
            for o in range(1, 4):
                back = bands[o][i, 0] * coef[0] + bands[o][i, 1] * coef[1] + bands[o][i, 2] * coef[2]
                product = product + pltpu.roll(back, o, 1)
                for k in range(3):
                    product = product + bands[o][i, k] * ahead[o - 1][k]
            fresh.append(jnp.where(inside, coef[i] + scale[i] * (rhs[i] - product), 0.0))
        coef = fresh
    cp[:, 3:4, :] = jnp.zeros((2, 1, 128), F32)
    for i in range(3):
        moved = pltpu.roll(coef[i], 384 - HALO, 1)
        for t in range(2):
            cp[t, i : i + 1] = moved[0:1, t * 128 : (t + 1) * 128]
    for i, k in enumerate(steps32):
        send(cp, cb.at[pl.ds(2 * pid, 2)], cg_s, cg_r, plane(*k))
    for t in range(2):
        cb[2 * pid + t] = cp[t]
    cb[BLOCKS] = jnp.zeros((4, 128), F32)
    settle(cb.at[0:62], cg_r)
    att_o[...] = cb[src][0:3]
    att_out = pltpu.make_async_copy(att_o, att_h, out_sem.at[1])
    att_out.start()

    def final_step(t, carry):
        for pair in range(LONG // 2):
            p = t * (LONG // 2) + pair
            halves = []
            for b in range(2):
                d = 2 * p + b
                now = jnp.concatenate([cb[d], cb[d + 1]], 0)
                turned = [now] + [pltpu.roll(now, 128 - j, 1) for j in range(1, 4)]
                flip = [pltpu.roll(v, 4, 0) for v in turned]
                pair01 = jnp.where(
                    upper, now, jnp.where(lane < 127, flip[1], turned[1])
                )
                pair23 = jnp.where(
                    upper,
                    jnp.where(lane < 126, turned[2], flip[2]),
                    jnp.where(lane < 125, flip[3], turned[3]),
                )
                stacked = jnp.concatenate([pair01, pair23], 0)
                halves.append(jnp.concatenate(parts(stacked, 3), 0).astype(BF16))
            both = jnp.concatenate(halves, 1)
            picked = dot(both, otk[p], NN)
            picked = picked[0:16] + picked[16:32] + picked[32:48]
            for b in range(2):
                d = 2 * p + b
                own = picked[:, b * 128 : b * 128 + 128]
                b01 = jnp.where(upper, bb[0, pl.ds(d, 1), :], bb[1, pl.ds(d, 1), :])
                b23 = jnp.where(upper, bb[2, pl.ds(d, 1), :], bb[3, pl.ds(d, 1), :])
                terms = ax8[:, cols(d)] * (own[0:8] * b01 + own[8:16] * b23)
                predicted = jnp.sum(terms, 0, keepdims=True)
                res_o[pl.ds(d, 1), :] = jnp.where(
                    lane1 < cnt[0, d], resid[pl.ds(d, 1), :] - predicted, 0.0
                )
        return carry

    lax.fori_loop(0, BLOCKS // LONG, final_step, 0)
    res_out = pltpu.make_async_copy(res_o, res_h, out_sem.at[2])
    res_out.start()

    settle(momr, ma_s)
    settle(par.at[0:7], pa_s)
    settle(nhalf, nh_s)
    settle(nr, np_s)
    settle(rhalf, rh_s)
    settle(rr, rp_s)
    settle(rz, rz_s)
    settle(cb.at[0:62], cg_s)

    @pl.when(is_owner)
    def _():
        settle(nz.at[0:6], nz_s)
        settle(rz, ng_s)

    @pl.when(jnp.logical_not(is_owner))
    def _():
        settle(nz.at[0:7], nz_s)

    for copy in (params_out, att_out, res_out):
        copy.wait()


def write_out(params_i, att_i, res_i, params_o, att_o, res_o, params, attitude, residual, sems):
    held = (params, attitude, residual)
    inward = [pltpu.make_async_copy(a, b, sems.at[i]) for i, (a, b) in enumerate(zip((params_i, att_i, res_i), held))]
    outward = [pltpu.make_async_copy(a, b, sems.at[i + 3]) for i, (a, b) in enumerate(zip(held, (params_o, att_o, res_o)))]
    for copy in inward:
        copy.start()
    for there, back in zip(inward, outward):
        there.wait()
        back.start()
    for copy in outward:
        copy.wait()


def on_device(design, observed, weight, phase_frac, axis_factors, source_index, knot_index, counts):
    dma = pltpu.SemaphoreType.DMA
    vm = lambda *shape: pltpu.VMEM(shape, F32)
    square = lambda v: v.reshape(64, 128)
    params, attitude, residual = pl.pallas_call(
        kernel,
        out_shape=(
            jax.ShapeDtypeStruct((5, 1024), F32),
            jax.ShapeDtypeStruct((3, 128), F32),
            jax.ShapeDtypeStruct((64, 128), F32),
        ),
        in_specs=[pl.BlockSpec(memory_space=pl.ANY)] * 8,
        out_specs=(pl.BlockSpec(memory_space=pl.ANY),) * 3,
        scratch_shapes=[
            vm(5, 1024), vm(3, 128), vm(64, 128), dma((3,)),
            vm(5, 8192), vm(64, 128), vm(64, 128), vm(64, 128), vm(3, 8192),
            pltpu.VMEM((64, 128), jnp.int32), pltpu.VMEM((64, 128), jnp.int32), pltpu.SMEM((1, 64), jnp.int32), dma((8,)),
            pltpu.VMEM((256, 8192), BF16),
            pltpu.VMEM((32, 256, 256), BF16),
            vm(14, 64, 128), vm(64, 128), vm(8, 8192),
            vm(256, 256), vm(8, 24, 128), vm(7, 24, 128), vm(8, 8, 128),
            vm(TILES, 24, 128), vm(HALF, 24, 128), vm(16, 7, 8, 128), vm(15, 7, 8, 128),
            vm(7, 8, 128), vm(8, 8, 128), vm(7, 8, 128), vm(14, 8, 128),
            vm(TILES, 4, 128), vm(HALF, 4, 128), vm(16, 3, 4, 128), vm(15, 3, 4, 128),
            vm(8, 128), vm(15, 8, 128), vm(2, 4, 128), vm(TILES, 4, 128), vm(64, 128),
        ]
        + [dma] * 20
        + [pltpu.SemaphoreType.REGULAR] * 2,
        compiler_params=pltpu.CompilerParams(
            collective_id=0, has_side_effects=True, vmem_limit_bytes=60 * 1024 * 1024
        ),
    )(
        design, square(observed), square(weight), square(phase_frac), axis_factors,
        square(source_index), square(knot_index), counts.reshape(1, 64),
    )
    anywhere = pl.BlockSpec(memory_space=pl.ANY)
    params, attitude, residual = pl.pallas_call(
        write_out,
        out_shape=(
            jax.ShapeDtypeStruct((5, 1024), F32),
            jax.ShapeDtypeStruct((3, 128), F32),
            jax.ShapeDtypeStruct((64, 128), F32),
        ),
        in_specs=[anywhere] * 3,
        out_specs=(anywhere,) * 3,
        scratch_shapes=[vm(5, 1024), vm(3, 128), vm(64, 128), dma((6,))],
        compiler_params=pltpu.CompilerParams(vmem_limit_bytes=60 * 1024 * 1024),
    )(params, attitude, residual)
    return params, attitude, residual.reshape(8192)


def solution(mesh):
    rows = P(("src", "ccd"))
    wide = P(None, ("src", "ccd"))
    in_specs = (wide, rows, rows, rows, wide, rows, rows, P("src", "ccd", None))
    out_specs = (P(None, "src"), P(None, "src"), rows)
    return jax.shard_map(on_device, mesh=mesh, in_specs=in_specs, out_specs=out_specs, check_vma=False)
```
